256 devices in a mesh: rows: 8 (over z), centers: 32 (over y, x, core).
Axes of the slice: x: 4, y: 4, z: 8, core: 2. Of those that a mesh axis runs over, the one named last changes fastest.
Arguments:
- features: float32 [8192, 128], P('rows'), may hold values from -6 to 6
- centers: float32 [16384, 128], P('centers'), may hold values from -6 to 6
- labels: int32 [8192, 64], P('rows'), may hold values 0 or 1
- coeffs: float32 [16384, 64], P('centers'), may hold values from -3 to 3
- precond: float32 [16384, 16384], P('rows', 'centers'), may hold values from -2 to 2, as said below
Outputs:
- coeffs_out: float32 [16384, 64], P('centers')
The draws below stay inside these ranges and needn't reach their ends.
Inputs may be any that keep to these rules, and one draw needn't show every extreme that they name: precond is lower triangular: every entry above the diagonal is zero, and its diagonal is positive.
All inputs are finite; a program needn't handle non-finite values. No bound on the sum of `labels` on one device may be relied on, other than what follows from the above.
Results may differ from the reference program's by a relative error of at most 0.0003.
Values sent between devices are 32-bit elements; how exact they have to be, the bound alone decides.
A program may use at most 64 MiB of HBM per device.

```python
import jax
import jax.numpy as jnp
from jax import lax

D = 128
M = 16384
OUT = 64
STEPS = 2
ROWS_ALL = 8192


def draw_precond(key, part):
    first = jax.random.fold_in(key, 11)
    second = jax.random.fold_in(key, 23)
    lower = jnp.clip(jax.random.normal(first, (M, M), jnp.float32), -6.0, 6.0) * (1.5 / jnp.sqrt(jnp.float32(M)))
    diag_vals = jnp.exp(jax.random.uniform(second, (M,), jnp.float32, jnp.log(0.5), jnp.log(2.0)))
    return jnp.tril(lower, -1) + jnp.diag(diag_vals)


def place_ends(drawn, key, least, top_value):
    shape = drawn.shape
    place = [jax.random.randint(jax.random.fold_in(key, axis), (), 0, shape[axis]) for axis in range(len(shape))]
    drawn = drawn.at[tuple(place)].set(least)
    longest = shape.index(max(shape))
    place[longest] = (place[longest] + 1) % shape[longest]
    return drawn.at[tuple(place)].set(top_value)


def levels(key, shape, shards, least, top_value):
    def one(position, blocks):
        heights = jax.random.uniform(jax.random.fold_in(jax.random.fold_in(key, 6), position), (blocks,), jnp.float32, least / len(shards), top_value / len(shards))
        return jnp.repeat(jnp.exp(heights), shape[position] // blocks).reshape((-1,) + (1,) * (len(shape) - position - 1))

    gain = one(*shards[0])
    for cut in shards[1:]:
        gain = gain * one(*cut)
    return gain


def scatter_about(key, shape, spread, limit, shards=(), kind=jnp.bfloat16):
    factor_of = levels(key, shape, shards, -0.22, 0.18) if shards else 1.0
    result = jax.random.normal(key, shape, jnp.float32) * spread * factor_of
    return jnp.minimum(jnp.maximum(result, -limit), limit).astype(kind)


def setup_inputs(seed: int = 0) -> dict:
    seeds = jax.random.split(jax.random.key(seed), 6)
    return {
        "features": scatter_about(seeds[0], (ROWS_ALL, D), 1.0, 6.0, ((0, 8),), jnp.float32),
        "centers": scatter_about(seeds[1], (M, D), 1.0, 6.0, ((0, 32),), jnp.float32),
        "labels": place_ends((jax.random.randint(seeds[2], (ROWS_ALL, OUT), 0, 2) < 1).astype(jnp.int32), jax.random.fold_in(seeds[2], 1), 0, 1),
        "coeffs": scatter_about(seeds[3], (M, OUT), 0.5, 3.0, ((0, 32),), jnp.float32),
        "precond": draw_precond(jax.random.fold_in(seeds[5], 71), 0),
    }


def kernel_tile(rows_x, centers_x):
    width = rows_x.shape[1]
    left = lax.optimization_barrier(jnp.sum(rows_x * rows_x, axis=1))
    right = lax.optimization_barrier(jnp.sum(centers_x * centers_x, axis=1))
    cross = jnp.dot(rows_x, centers_x.T, precision=lax.Precision.HIGHEST)
    return jnp.exp(-2.0 * (left[:, None] + right[None, :] - 2.0 * cross) / width)

def reference(features, centers, labels, coeffs, precond):
    rows_total = features.shape[0]
    block = min(1024, rows_total)
    blocks = rows_total // block
    targets = labels.astype(jnp.float32)
    for step in range(STEPS):

        def accumulate(total, index):
            start = (index * block).astype(jnp.int32)
            rows_x = lax.dynamic_slice_in_dim(features, start, block, 0)
            rows_y = lax.dynamic_slice_in_dim(targets, start, block, 0)
            tile = kernel_tile(rows_x, centers)
            logits = jnp.dot(tile, coeffs, precision=lax.Precision.HIGHEST)
            resid = (jax.nn.sigmoid(logits) - rows_y) / rows_total
            return (total + jnp.dot(tile.T, resid, precision=lax.Precision.HIGHEST), None)
        grad, unused = lax.scan(accumulate, jnp.zeros(coeffs.shape, jnp.float32), jnp.arange(blocks, dtype=jnp.int32))
        fwd = jnp.dot(precond, grad, precision=lax.Precision.HIGHEST)
        back = jnp.dot(precond.T, fwd, precision=lax.Precision.HIGHEST)
        total = jnp.sum(fwd * fwd)
        scale = 0.5 / jnp.sqrt(total / (fwd.shape[0] * fwd.shape[1]) + 1e-06)
        coeffs = coeffs - scale * back
    return coeffs
```

```python
import functools

import jax
import jax.numpy as jnp
from jax import lax
from jax.experimental import pallas as pl
from jax.experimental.pallas import tpu as pltpu
from jax.sharding import PartitionSpec as P

STEPS = 2
step_size = 0.5
epsilon = 1e-06

Z, Y, X = 8, 4, 4
CHIPS = Y * X
D = 128
OUT = 64
OUTS = OUT // 2
GROUPS = OUTS // 8
ROWS = 1024
CENT = 512
PROWS = 2048
RS_ROWS = ROWS // X
RS_PROWS = PROWS // X
FAR_FIRST = (2, 1, 3, 0)
Z_EVEN = (4, 2, 6)
Z_ODD = (3, 5, 1, 7)
f32 = jnp.float32
bf16 = jnp.bfloat16
MESH = pl.DeviceIdType.MESH


def split(x):
    hi = x.astype(bf16)
    lo = (x - hi.astype(f32)).astype(bf16)
    return hi, lo


def stacked(x):
    hi, lo = split(x)
    return jnp.concatenate([hi, lo], axis=0), hi


def product(lhs, w_hi, w_lo, contract):
    both, hi = lhs
    dims = (((1,), (contract,)), ((), ()))
    r = lax.dot_general(both, w_hi, dims, preferred_element_type=f32)
    s = lax.dot_general(hi, w_lo, dims, preferred_element_type=f32)
    return r[:OUTS] + r[OUTS:] + s


def kernel(
    feat_hbm, cent_hbm, lab_hbm, coef_hbm, prec_hbm, out_ref,
    feat, cent, lab, labt, coef, coeft, k_hi, k_lo, p_raw, p_hi, p_lo,
    log_p, log_r, res_f, gra_p, gra_r, gra_f, fwd_p, fwd_r, fwd_f, bak_p, bak_r, a_f, sq_s, sq_r, fin_s, fin_r,
    load_sem, pair_send, pair_recv,
    log_ss, log_rs, res_ss, res_rs, gra_ss, gra_rs, grf_ss, grf_rs,
    fwd_ss, fwd_rs, fwf_ss, fwf_rs, bak_ss, bak_rs, af_ss, af_rs,
):
    z = lax.axis_index("rows")
    c = lax.axis_index("centers")
    j = c // 2
    k = c % 2
    y = j // X
    x = j % X
    zlo = z % 2
    partner = c + 1 - 2 * k
    my_rg = x

    lab_row = pl.multiple_of(x * RS_ROWS, RS_ROWS)
    loads = [
        pltpu.make_async_copy(feat_hbm, feat, load_sem.at[0]),
        pltpu.make_async_copy(cent_hbm, cent.at[k], load_sem.at[1]),
        pltpu.make_async_copy(coef_hbm, coef.at[k], load_sem.at[2]),
        pltpu.make_async_copy(lab_hbm.at[pl.ds(lab_row, RS_ROWS), :], lab, load_sem.at[3]),
        pltpu.make_async_copy(prec_hbm, p_raw.at[k], load_sem.at[4]),
    ]
    for copy in loads:
        copy.start()

    barrier = pltpu.get_barrier_semaphore()
    pl.semaphore_signal(barrier, inc=1, device_id=(z, partner), device_id_type=MESH)

    def chip_at(dy, dx):
        return lax.rem(y + dy, Y) * X + lax.rem(x + dx, X)

    plane = [(dy, dx) for dx in FAR_FIRST for dy in FAR_FIRST if (dy, dx) != (0, 0)]
    for dy, dx in plane:
        pl.semaphore_signal(barrier, inc=1, device_id=(z, 2 * chip_at(dy, dx) + k), device_id_type=MESH)
    for oz in Z_EVEN + Z_ODD:
        pl.semaphore_signal(barrier, inc=1, device_id=(lax.rem(z + oz, Z), c), device_id_type=MESH)

    def remote(src, dst, send, recv, device):
        return pltpu.make_async_remote_copy(
            src_ref=src, dst_ref=dst, send_sem=send, recv_sem=recv, device_id=device, device_id_type=MESH
        )

    def to_plane(src, dst, ss, rs, dy, dx):
        o = dy * X + dx
        return remote(src, dst, ss.at[o], rs.at[o], (z, 2 * chip_at(dy, dx) + k))

    def to_z(src, dst, ss, rs, oz):
        return remote(src, dst, ss.at[oz], rs.at[oz], (lax.rem(z + oz, Z), c))

    loads[0].wait()
    loads[1].wait()
    fx = feat[...]
    row_norm = lax.dot_general(
        jnp.ones((8, D), f32), fx * fx, (((1,), (1,)), ((), ())),
        precision=lax.Precision.HIGHEST, preferred_element_type=f32,
    )[:1]

    def kernel_half(h):
        @pl.loop(0, CENT // 128)
        def _(i):
            at = pl.multiple_of(i * 128, 128)
            cx = cent[h, pl.ds(at, 128), :]
            cn = jnp.sum(cx * cx, axis=1, keepdims=True)
            cross = lax.dot_general(
                cx, feat[...], (((1,), (1,)), ((), ())),
                precision=lax.Precision.HIGHEST, preferred_element_type=f32,
            )
            tile = jnp.exp(-2.0 * (cn + row_norm - 2.0 * cross) / D)
            hi, lo = split(tile)
            k_hi[h, pl.ds(at, 128), :] = hi
            k_lo[h, pl.ds(at, 128), :] = lo

    kernel_half(k)
    loads[2].wait()
    coeft[k] = coef[k].T

    pl.semaphore_wait(barrier, 1 + len(plane) + Z - 1)
    cent_pair = remote(cent_hbm, cent.at[k], pair_send.at[0], pair_recv.at[0], (z, partner))
    coef_pair = remote(coef_hbm, coef.at[k], pair_send.at[1], pair_recv.at[1], (z, partner))
    prec_pair = remote(prec_hbm, p_raw.at[k], pair_send.at[2], pair_recv.at[2], (z, partner))
    cent_pair.start()
    coef_pair.start()
    prec_pair.start()
    other = 1 - k
    loads[3].wait()
    labt[...] = lab[...].astype(f32).T
    cent_pair.wait()
    kernel_half(other)
    coef_pair.wait()
    coeft[other] = coef[other].T
    for og in range(GROUPS):
        at = pl.multiple_of(k * OUTS + og * 8, 8)
        for h in range(2):
            a_f[og * 2 + h] = coeft[h, pl.ds(at, 8), :]
    targets = labt[pl.ds(pl.multiple_of(k * OUTS + y * 8, 8), 8), :]

    def half_of(pieces, h):
        return jnp.concatenate([pieces[og * 2 + h] for og in range(GROUPS)], axis=0)

    def line_of(pieces):
        return jnp.concatenate(
            [
                jnp.concatenate([pieces[og * X + rg] for rg in range(X)], axis=1)
                for og in range(GROUPS)
            ],
            axis=0,
        )

    def precond_half(h):
        @pl.loop(0, PROWS // 128)
        def _(i):
            at = pl.multiple_of(i * 128, 128)
            hi, lo = split(p_raw[h, pl.ds(at, 128), :])
            p_hi[h, pl.ds(at, 128), :] = hi
            p_lo[h, pl.ds(at, 128), :] = lo

    for step in range(STEPS):
        lhs = [stacked(half_of(a_f, h)) for h in range(2)]
        sends = []
        for dx in FAR_FIRST:
            rg = lax.rem(x + dx, X)
            at = pl.ds(pl.multiple_of(rg * RS_ROWS, RS_ROWS), RS_ROWS)
            part = product(lhs[0], k_hi[0, :, at], k_lo[0, :, at], 0) + product(
                lhs[1], k_hi[1, :, at], k_lo[1, :, at], 0
            )
            for og in range(GROUPS):
                log_p[og * X + rg] = part[og * 8 : og * 8 + 8]
            for dy in FAR_FIRST:
                if (dy, dx) != (0, 0):
                    copy = to_plane(log_p.at[chip_at(dy, dx)], log_r.at[dy * X + dx], log_ss, log_rs, dy, dx)
                    copy.start()
                    sends.append(copy)
        if step == 0:
            loads[4].wait()
            precond_half(k)
        total = log_p[j]
        for copy, (dy, dx) in reversed(list(zip(sends, plane))):
            copy.wait_recv()
            total = total + log_r[dy * X + dx]
        res_f[j] = (jax.nn.sigmoid(total) - targets) * (1.0 / (ROWS * Z))

        gathers = []
        for dy, dx in plane:
            copy = to_plane(res_f.at[j], res_f.at[j], res_ss, res_rs, dy, dx)
            copy.start()
            gathers.append(copy)
        if step == 0:
            prec_pair.wait()
            precond_half(other)
        for copy in sends:
            copy.wait_send()
        for copy in reversed(gathers):
            copy.wait_recv()
        lhs = stacked(line_of(res_f))
        for copy in gathers:
            copy.wait_send()

        sends = []
        for rel, offsets in ((0, Z_EVEN), (1, Z_ODD)):
            cg = lax.rem(zlo + rel, 2)
            for s in range(2):
                at = slice(s * 256, s * 256 + 256)
                part = product(lhs, k_hi[cg, at, :], k_lo[cg, at, :], 1)
                for og in range(GROUPS):
                    gra_p[og * 2 + cg, :, at] = part[og * 8 : og * 8 + 8]
            for oz in offsets:
                copy = to_z(gra_p.at[lax.rem(z + oz, Z)], gra_r.at[oz], gra_ss, gra_rs, oz)
                copy.start()
                sends.append((oz, copy))
        total = gra_p[z]
        for oz, copy in reversed(sends):
            copy.wait_recv()
            total = total + gra_r[oz]
        gra_f[z] = total
        gathers = []
        for oz in Z_EVEN + Z_ODD:
            copy = to_z(gra_f.at[z], gra_f.at[z], grf_ss, grf_rs, oz)
            copy.start()
            gathers.append(copy)
        for oz, copy in sends:
            copy.wait_send()
        for copy in reversed(gathers):
            copy.wait_recv()
        lhs = [stacked(half_of(gra_f, h)) for h in range(2)]
        for copy in gathers:
            copy.wait_send()

        sends = []
        for dx in FAR_FIRST:
            rg = lax.rem(x + dx, X)
            for s in range(2):
                at = pl.ds(pl.multiple_of(rg * RS_PROWS + s * 256, 256), 256)
                part = product(lhs[0], p_hi[0, at, :], p_lo[0, at, :], 1) + product(
                    lhs[1], p_hi[1, at, :], p_lo[1, at, :], 1
                )
                for og in range(GROUPS):
                    fwd_p[og * X + rg, :, s * 256 : s * 256 + 256] = part[og * 8 : og * 8 + 8]
            for dy in FAR_FIRST:
                if (dy, dx) != (0, 0):
                    copy = to_plane(fwd_p.at[chip_at(dy, dx)], fwd_r.at[dy * X + dx], fwd_ss, fwd_rs, dy, dx)
                    copy.start()
                    sends.append(copy)
        total = fwd_p[j]
        for copy, (dy, dx) in reversed(list(zip(sends, plane))):
            copy.wait_recv()
            total = total + fwd_r[dy * X + dx]
        fwd_f[j] = total
        gathers = []
        for dy, dx in plane:
            copy = to_plane(fwd_f.at[j], fwd_f.at[j], fwf_ss, fwf_rs, dy, dx)
            copy.start()
            gathers.append(copy)
        for copy in sends:
            copy.wait_send()
        for copy in reversed(gathers):
            copy.wait_recv()
        square = jnp.zeros((8, RS_PROWS), f32)
        for i in range(CHIPS):
            square = square + fwd_f[i] * fwd_f[i]
        square = square[:, :256] + square[:, 256:]
        square = square[:, :128] + square[:, 128:]
        sq_s[step] = square
        sq_pair = remote(
            sq_s.at[step], sq_r.at[step], pair_send.at[3 + step], pair_recv.at[3 + step], (z, partner)
        )
        sq_pair.start()
        lhs = stacked(line_of(fwd_f))
        for copy in gathers:
            copy.wait_send()

        def back_part(cg):
            for s in range(2):
                at = slice(s * 256, s * 256 + 256)
                part = product(lhs, p_hi[cg, :, at], p_lo[cg, :, at], 0)
                for og in range(GROUPS):
                    bak_p[og * 2 + cg, :, at] = part[og * 8 : og * 8 + 8]

        sends = []
        for rel, offsets in ((0, Z_EVEN), (1, Z_ODD)):
            cg = lax.rem(zlo + rel, 2)
            back_part(cg)
            if rel == 0:
                sq_pair.wait()
                square = square + sq_r[step]
                for i in range(Z):
                    bak_p[i, :, CENT:] = square
            for oz in offsets:
                copy = to_z(bak_p.at[lax.rem(z + oz, Z)], bak_r.at[oz], bak_ss, bak_rs, oz)
                copy.start()
                sends.append((oz, copy))
        total = bak_p[z]
        for oz, copy in reversed(sends):
            copy.wait_recv()
            total = total + bak_r[oz]
        squares = jnp.sum(jnp.sum(total[:, CENT:], axis=1, keepdims=True), axis=0, keepdims=True)
        scale = step_size / jnp.sqrt(squares / (CENT * 2 * CHIPS * OUT) + epsilon)
        a_f[z] = a_f[z] - scale * total[:, :CENT]
        gathers = []
        for oz in Z_EVEN + Z_ODD:
            copy = to_z(a_f.at[z], a_f.at[z], af_ss, af_rs, oz)
            copy.start()
            gathers.append(copy)
        for oz, copy in sends:
            copy.wait_send()
        for copy in reversed(gathers):
            copy.wait_recv()
        for copy in gathers:
            copy.wait_send()

    for og in range(GROUPS):
        fin_s[og] = a_f[og * 2 + other]
    fin_pair = remote(fin_s, fin_r, pair_send.at[5], pair_recv.at[5], (z, partner))
    fin_pair.start()
    mine = pl.multiple_of(k * OUTS, OUTS)
    theirs = pl.multiple_of(other * OUTS, OUTS)
    for og in range(GROUPS):
        out_ref[pl.ds(mine + og * 8, 8), :] = a_f[og * 2 + k]
    fin_pair.wait()
    for og in range(GROUPS):
        out_ref[pl.ds(theirs + og * 8, 8), :] = fin_r[og]


def body(features, centers, labels, coeffs, precond):
    any_space = pl.BlockSpec(memory_space=pl.ANY)
    V = pltpu.VMEM
    dma = pltpu.SemaphoreType.DMA
    scratch = [
        V((ROWS, D), f32),
        V((2, CENT, D), f32),
        V((RS_ROWS, OUT), jnp.int32),
        V((OUT, RS_ROWS), f32),
        V((2, CENT, OUT), f32),
        V((2, OUT, CENT), f32),
        V((2, CENT, ROWS), bf16),
        V((2, CENT, ROWS), bf16),
        V((2, PROWS, CENT), f32),
        V((2, PROWS, CENT), bf16),
        V((2, PROWS, CENT), bf16),
        V((CHIPS, 8, RS_ROWS), f32),
        V((CHIPS, 8, RS_ROWS), f32),
        V((CHIPS, 8, RS_ROWS), f32),
        V((Z, 8, CENT), f32),
        V((Z, 8, CENT), f32),
        V((Z, 8, CENT), f32),
        V((CHIPS, 8, RS_PROWS), f32),
        V((CHIPS, 8, RS_PROWS), f32),
        V((CHIPS, 8, RS_PROWS), f32),
        V((Z, 8, CENT + 128), f32),
        V((Z, 8, CENT + 128), f32),
        V((Z, 8, CENT), f32),
        V((STEPS, 8, 128), f32),
        V((STEPS, 8, 128), f32),
        V((GROUPS, 8, CENT), f32),
        V((GROUPS, 8, CENT), f32),
        dma((5,)),
        dma((6,)),
        dma((6,)),
    ]
    for count in (CHIPS, CHIPS, Z, Z, CHIPS, CHIPS, Z, Z):
        scratch += [dma((count,)), dma((count,))]
    out = pl.pallas_call(
        kernel,
        out_shape=jax.ShapeDtypeStruct((OUT, CENT), f32),
        in_specs=[any_space] * 5,
        out_specs=pl.BlockSpec(memory_space=pltpu.VMEM),
        scratch_shapes=scratch,
        compiler_params=pltpu.CompilerParams(
            collective_id=0, has_side_effects=True, vmem_limit_bytes=60 * 1024 * 1024
        ),
        name="falkon",
    )(features, centers, labels, coeffs, precond)
    return out.T


def solution(mesh):
    in_specs = (
        P("rows", None),
        P("centers", None),
        P("rows", None),
        P("centers", None),
        P("rows", "centers"),
    )
    return jax.shard_map(body, mesh=mesh, in_specs=in_specs, out_specs=P("centers", None), check_vma=False)
```

```python
import functools

import jax
import jax.numpy as jnp
from jax import lax
from jax.experimental import pallas as pl
from jax.experimental.pallas import tpu as pltpu
from jax.sharding import PartitionSpec as P

STEPS = 2
step_size = 0.5
epsilon = 1e-06
LOG2E = 1.4426950408889634

Z, Y, X = 8, 4, 4
CHIPS = Y * X
D = 128
OUT = 64
OUTS = OUT // 2
GROUPS = OUTS // 8
ROWS = 1024
CENT = 512
PROWS = 2048
RS_ROWS = ROWS // X
RS_PROWS = PROWS // X
FAR_FIRST = (2, 1, 3, 0)
NEAR_FIRST = (0, 1, 3, 2)
Z_EVEN = (4, 2, 6)
Z_ODD = (3, 5, 1, 7)
f32 = jnp.float32
bf16 = jnp.bfloat16
MESH = pl.DeviceIdType.MESH


def split(x):
    hi = x.astype(bf16)
    lo = (x - hi.astype(f32)).astype(bf16)
    return hi, lo


def split3(x):
    hi = x.astype(bf16)
    rest = x - hi.astype(f32)
    mid = rest.astype(bf16)
    lo = (rest - mid.astype(f32)).astype(bf16)
    return hi, mid, lo


def stacked(x):
    hi, lo = split(x)
    return jnp.concatenate([hi, lo], axis=0), hi


def dot(a, b, contract):
    return lax.dot_general(a, b, (((1,), (contract,)), ((), ())), preferred_element_type=f32)


def product(lhs, w_hi, w_lo, contract):
    both, hi = lhs
    n = hi.shape[0]
    r = dot(both, w_hi, contract)
    s = dot(hi, w_lo, contract)
    return r[:n] + r[n:] + s


def kernel(
    feat_hbm, cent_hbm, lab_hbm, coef_hbm, prec_hbm, out_ref,
    feat, cent, lab, coef, coef_pair, r1, r2, r3, l1, l2, norm, k_hi, k_lo, p_raw, p_hi, p_lo,
    pair_s, pair_r, log_a, gra_a, fwd_a, bak_a,
    log_p, log_r, res_f, gra_p, gra_r, gra_f, fwd_p, fwd_r, fwd_f, bak_p, bak_r, a_f, sq_s, sq_r, fin,
    load_sem, pair_send, pair_recv, pch_send, pch_recv,
    log_ss, log_rs, res_ss, res_rs, gra_ss, gra_rs, grf_ss, grf_rs,
    fwd_ss, fwd_rs, fwf_ss, fwf_rs, bak_ss, bak_rs, af_ss, af_rs, sq_ss, sq_rs, fin_ss, fin_rs,
):
    z = lax.axis_index("rows")
    c = lax.axis_index("centers")
    j = c // 2
    k = c % 2
    y = j // X
    x = j % X
    zlo = z % 2
    other = 1 - k
    partner = c + 1 - 2 * k
    mine = pl.multiple_of(k * OUTS, OUTS)
    theirs = pl.multiple_of(other * OUTS, OUTS)

    lab_at = (
        pl.ds(pl.multiple_of(k * OUTS + y * 8, 8), 8),
        pl.ds(pl.multiple_of(x * RS_ROWS, RS_ROWS), RS_ROWS),
    )
    loads = [
        pltpu.make_async_copy(feat_hbm, feat, load_sem.at[0]),
        pltpu.make_async_copy(cent_hbm, cent.at[k], load_sem.at[1]),
        pltpu.make_async_copy(coef_hbm, coef, load_sem.at[2]),
        pltpu.make_async_copy(lab_hbm.at[lab_at], lab, load_sem.at[3]),
        pltpu.make_async_copy(prec_hbm, p_raw.at[k], load_sem.at[4]),
    ]
    for copy in loads:
        copy.start()

    barrier = pltpu.get_barrier_semaphore()
    pl.semaphore_signal(barrier, inc=1, device_id=(z, partner), device_id_type=MESH)

    def chip_at(dy, dx):
        return lax.rem(y + dy, Y) * X + lax.rem(x + dx, X)

    plane = [(dy, dx) for dx in FAR_FIRST for dy in FAR_FIRST if (dy, dx) != (0, 0)]
    for dy, dx in plane:
        pl.semaphore_signal(barrier, inc=1, device_id=(z, 2 * chip_at(dy, dx) + k), device_id_type=MESH)
    for oz in Z_EVEN + Z_ODD:
        pl.semaphore_signal(barrier, inc=1, device_id=(lax.rem(z + oz, Z), c), device_id_type=MESH)
        pl.semaphore_signal(barrier, inc=1, device_id=(lax.rem(z + oz, Z), partner), device_id_type=MESH)

    def remote(src, dst, send, recv, device):
        return pltpu.make_async_remote_copy(
            src_ref=src, dst_ref=dst, send_sem=send, recv_sem=recv, device_id=device, device_id_type=MESH
        )

    def to_pair(src, dst, n):
        return remote(src, dst, pair_send.at[n], pair_recv.at[n], (z, partner))

    def to_plane(src, dst, ss, rs, dy, dx):
        o = dy * X + dx
        return remote(src, dst, ss.at[o], rs.at[o], (z, 2 * chip_at(dy, dx) + k))

    def to_z(src, dst, ss, rs, oz):
        return remote(src, dst, ss.at[oz], rs.at[oz], (lax.rem(z + oz, Z), c))

    factor = 2.0 * LOG2E / D
    loads[0].wait()
    fx = feat[...]
    hi, mid, lo = split3(fx)
    r1[...] = jnp.concatenate([hi, hi], axis=1)
    r2[...] = jnp.concatenate([mid, mid], axis=1)
    r3[...] = jnp.concatenate([lo, hi], axis=1)
    hi, mid, lo = split3(fx * fx)
    ones = jnp.ones((16, D), bf16)
    row_norm = dot(ones, hi, 1) + dot(ones, mid, 1) + dot(ones, lo, 1)
    norm[...] = row_norm[:8] * factor

    def kernel_half(h):
        cx = cent[h]
        hi, mid, lo = split3(cx)
        l1[...] = jnp.concatenate([hi, mid], axis=1)
        l2[...] = jnp.concatenate([hi, lo], axis=1)
        cn = jnp.sum(cx * cx, axis=1, keepdims=True) * factor

        @pl.loop(0, X)
        def _(i):
            at = pl.ds(pl.multiple_of(i * RS_ROWS, RS_ROWS), RS_ROWS)
            cross = dot(l1[...], r1[at, :], 1) + dot(l1[...], r2[at, :], 1) + dot(l2[...], r3[at, :], 1)
            tile = jnp.exp2(cross * (2.0 * factor) - (cn + norm[:1, at]))
            hi, lo = split(tile)
            k_hi[h, :, at] = hi
            k_lo[h, :, at] = lo

    def precond_half(h):
        @pl.loop(0, PROWS // 128)
        def _(i):
            at = pl.multiple_of(i * 128, 128)
            hi, lo = split(p_raw[h, pl.ds(at, 128), :])
            p_hi[h, pl.ds(at, 128), :] = hi
            p_lo[h, pl.ds(at, 128), :] = lo

    precond_chunks = [
        remote(
            p_raw.at[k, pl.ds(i * 256, 256), :], p_raw.at[k, pl.ds(i * 256, 256), :],
            pch_send.at[i], pch_recv.at[i], (z, partner),
        )
        for i in range(8)
    ]

    loads[1].wait()
    kernel_half(k)
    loads[2].wait()

    def half_of(pieces, h):
        return jnp.concatenate([pieces[og * 2 + h] for og in range(GROUPS)], axis=0)

    def line_of(pieces, rg):
        return jnp.concatenate([pieces[og * X + rg] for og in range(GROUPS)], axis=0)

    for step in range(STEPS):
        sends = []

        def send_logits(dx, part):
            rg = lax.rem(x + dx, X)
            for og in range(GROUPS):
                log_p[og * X + rg] = part[og * 8 : og * 8 + 8]
            for dy in FAR_FIRST:
                if (dy, dx) != (0, 0):
                    copy = to_plane(log_p.at[chip_at(dy, dx)], log_r.at[dy * X + dx], log_ss, log_rs, dy, dx)
                    copy.start()
                    sends.append(copy)

        def rows_at(dx):
            return pl.ds(pl.multiple_of(lax.rem(x + dx, X) * RS_ROWS, RS_ROWS), RS_ROWS)

        if step == 0:
            lhs = stacked(jnp.concatenate([coef[pl.ds(theirs, OUTS), :], coef[pl.ds(mine, OUTS), :]], axis=0))
            for n, dx in enumerate(FAR_FIRST):
                part = product(lhs, k_hi[k, :, rows_at(dx)], k_lo[k, :, rows_at(dx)], 0)
                pair_s[n] = part[:OUTS]
                log_a[n] = part[OUTS:]
            pl.semaphore_wait(barrier, 1 + len(plane) + 2 * (Z - 1))
            pairs = [to_pair(pair_s.at[n], pair_r.at[n], n) for n in range(X)]
            for copy in pairs:
                copy.start()
            cent_pair = to_pair(cent.at[k], cent.at[k], 4)
            cent_pair.start()
            coef_copy = to_pair(coef.at[pl.ds(theirs, OUTS), :], coef_pair, 5)
            coef_copy.start()
            for n, dx in enumerate(FAR_FIRST):
                pairs[n].wait_recv()
                send_logits(dx, log_a[n] + pair_r[n])
            loads[4].wait()
            for copy in precond_chunks[:4]:
                copy.start()
            for copy in pairs:
                copy.wait_send()
            cent_pair.wait()
            kernel_half(other)
            coef_copy.wait()
            for og in range(GROUPS):
                a_f[og * 2 + k] = coef[pl.ds(mine + og * 8, 8), :]
                a_f[og * 2 + other] = coef_pair[og * 8 : og * 8 + 8, :]
            precond_half(k)
            loads[3].wait()
        else:
            for rel, offsets in ((1, Z_ODD), (0, Z_EVEN)):
                for copy in gathers[rel]:
                    copy.wait_recv()
                h = lax.rem(zlo + rel, 2)
                lhs = stacked(half_of(a_f, h))
                for n, dx in enumerate(FAR_FIRST):
                    part = product(lhs, k_hi[h, :, rows_at(dx)], k_lo[h, :, rows_at(dx)], 0)
                    if rel:
                        log_a[n] = part
                    else:
                        send_logits(dx, log_a[n] + part)
            for rel in range(2):
                for copy in gathers[rel]:
                    copy.wait_send()
        total = log_p[j]
        for copy, (dy, dx) in reversed(list(zip(sends, plane))):
            copy.wait_recv()
            total = total + log_r[dy * X + dx]
        res_f[j] = (jax.nn.sigmoid(total) - lab[...].astype(f32)) * (1.0 / (ROWS * Z))

        gathers = {}
        for dy, dx in plane:
            copy = to_plane(res_f.at[j], res_f.at[j], res_ss, res_rs, dy, dx)
            copy.start()
            gathers.setdefault(dx, []).append(copy)
        if step == 0:
            for copy in precond_chunks[4:]:
                copy.start()
        for copy in sends:
            copy.wait_send()

        sends = []
        for dx in NEAR_FIRST:
            for copy in reversed(gathers[dx]):
                copy.wait_recv()
            rg = lax.rem(x - dx + X, X)
            lhs = stacked(line_of(res_f, rg))
            rows = pl.ds(pl.multiple_of(rg * RS_ROWS, RS_ROWS), RS_ROWS)
            for rel, offsets in ((0, Z_EVEN), (1, Z_ODD)):
                cg = lax.rem(zlo + rel, 2)
                for s in range(2):
                    at = slice(s * 256, s * 256 + 256)
                    part = product(lhs, k_hi[cg, at, rows], k_lo[cg, at, rows], 1)
                    if dx != NEAR_FIRST[0]:
                        part = gra_a[rel, :, at] + part
                    if dx != NEAR_FIRST[-1]:
                        gra_a[rel, :, at] = part
                    else:
                        for og in range(GROUPS):
                            gra_p[og * 2 + cg, :, at] = part[og * 8 : og * 8 + 8]
                if dx == NEAR_FIRST[-1]:
                    for oz in offsets:
                        copy = to_z(gra_p.at[lax.rem(z + oz, Z)], gra_r.at[oz], gra_ss, gra_rs, oz)
                        copy.start()
                        sends.append((oz, copy))
        for dx in NEAR_FIRST:
            for copy in gathers[dx]:
                copy.wait_send()
        if step == 0:
            for copy in precond_chunks:
                copy.wait()
            precond_half(other)
        total = gra_p[z]
        for oz, copy in reversed(sends):
            copy.wait_recv()
            total = total + gra_r[oz]
        gra_f[z] = total
        gathers = {0: [], 1: []}
        for oz in Z_EVEN + Z_ODD:
            copy = to_z(gra_f.at[z], gra_f.at[z], grf_ss, grf_rs, oz)
            copy.start()
            gathers[oz % 2].append(copy)
        for oz, copy in sends:
            copy.wait_send()

        sends = []
        for rel in (1, 0):
            for copy in gathers[rel]:
                copy.wait_recv()
            h = lax.rem(zlo + rel, 2)
            lhs = stacked(half_of(gra_f, h))
            for n, dx in enumerate(FAR_FIRST):
                rg = lax.rem(x + dx, X)
                for s in range(2):
                    at = pl.ds(pl.multiple_of(rg * RS_PROWS + s * 256, 256), 256)
                    col = slice(s * 256, s * 256 + 256)
                    part = product(lhs, p_hi[h, at, :], p_lo[h, at, :], 1)
                    if rel:
                        fwd_a[n, :, col] = part
                    else:
                        part = fwd_a[n, :, col] + part
                        for og in range(GROUPS):
                            fwd_p[og * X + rg, :, col] = part[og * 8 : og * 8 + 8]
                if not rel:
                    for dy in FAR_FIRST:
                        if (dy, dx) != (0, 0):
                            copy = to_plane(
                                fwd_p.at[chip_at(dy, dx)], fwd_r.at[dy * X + dx], fwd_ss, fwd_rs, dy, dx
                            )
                            copy.start()
                            sends.append(copy)
        for rel in range(2):
            for copy in gathers[rel]:
                copy.wait_send()
        total = fwd_p[j]
        for copy, (dy, dx) in reversed(list(zip(sends, plane))):
            copy.wait_recv()
            total = total + fwd_r[dy * X + dx]
        fwd_f[j] = total
        gathers = {}
        for dy, dx in plane:
            copy = to_plane(fwd_f.at[j], fwd_f.at[j], fwf_ss, fwf_rs, dy, dx)
            copy.start()
            gathers.setdefault(dx, []).append(copy)
        for copy in sends:
            copy.wait_send()

        sends = []
        square = jnp.zeros((8, 128), f32)
        for dx in NEAR_FIRST:
            for copy in reversed(gathers[dx]):
                copy.wait_recv()
            rg = lax.rem(x - dx + X, X)
            line = line_of(fwd_f, rg)
            for og in range(GROUPS):
                for t in range(RS_PROWS // 128):
                    tile = line[og * 8 : og * 8 + 8, t * 128 : t * 128 + 128]
                    square = square + tile * tile
            if dx == NEAR_FIRST[-1]:
                sq_s[step] = square
                for i in range(Z):
                    bak_p[i, :, CENT:] = square
                squares = [
                    remote(
                        sq_s.at[step], sq_r.at[step, oz], sq_ss.at[step, oz], sq_rs.at[step, oz],
                        (lax.rem(z + oz, Z), partner),
                    )
                    for oz in Z_EVEN + Z_ODD + (0,)
                ]
                for copy in squares:
                    copy.start()
            lhs = stacked(line)
            rows = pl.ds(pl.multiple_of(rg * RS_PROWS, RS_PROWS), RS_PROWS)
            for rel, offsets in ((0, Z_EVEN), (1, Z_ODD)):
                cg = lax.rem(zlo + rel, 2)
                for s in range(2):
                    at = slice(s * 256, s * 256 + 256)
                    part = product(lhs, p_hi[cg, rows, at], p_lo[cg, rows, at], 0)
                    if dx != NEAR_FIRST[0]:
                        part = bak_a[rel, :, at] + part
                    if dx != NEAR_FIRST[-1]:
                        bak_a[rel, :, at] = part
                    else:
                        for og in range(GROUPS):
                            bak_p[og * 2 + cg, :, at] = part[og * 8 : og * 8 + 8]
                if dx == NEAR_FIRST[-1]:
                    for oz in offsets:
                        copy = to_z(bak_p.at[lax.rem(z + oz, Z)], bak_r.at[oz], bak_ss, bak_rs, oz)
                        copy.start()
                        sends.append((oz, copy))
        for dx in NEAR_FIRST:
            for copy in gathers[dx]:
                copy.wait_send()
        total = bak_p[z]
        for oz, copy in reversed(sends):
            copy.wait_recv()
            total = total + bak_r[oz]
        square = total[:, CENT:]
        for copy in squares:
            copy.wait_recv()
        for oz in range(Z):
            square = square + sq_r[step, oz]
        square = jnp.sum(jnp.sum(square, axis=1, keepdims=True), axis=0, keepdims=True)
        scale = step_size / jnp.sqrt(square / (CENT * 2 * CHIPS * OUT) + epsilon)
        a_f[z] = a_f[z] - scale * total[:, :CENT]
        for copy in squares:
            copy.wait_send()
        if step < STEPS - 1:
            gathers = {0: [], 1: []}
            for oz in Z_EVEN + Z_ODD:
                copy = to_z(a_f.at[z], a_f.at[z], af_ss, af_rs, oz)
                copy.start()
                gathers[oz % 2].append(copy)
        for oz, copy in sends:
            copy.wait_send()

    og = z // 2
    rel = lax.rem(k + zlo, 2)
    piece = k * GROUPS + og

    def to_holder(oz, r):
        return remote(
            a_f.at[z], fin.at[piece], fin_ss.at[oz], fin_rs.at[oz * 2 + r], (lax.rem(z + oz, Z), 2 * j + zlo)
        )

    def from_holder(oz, r):
        source = (k + r * (1 - 2 * k)) * GROUPS + lax.rem(z - oz + Z, Z) // 2
        remote(a_f.at[z], fin.at[source], fin_ss.at[oz], fin_rs.at[oz * 2 + r], (z, partner)).wait_recv()

    copies = [to_holder(oz, rel) for oz in Z_EVEN + Z_ODD]
    for copy in copies:
        copy.start()

    @pl.when(rel == 0)
    def _():
        fin[piece] = a_f[z]
        from_holder(0, 1)
        for oz in Z_EVEN:
            for r in range(2):
                from_holder(oz, r)

    @pl.when(rel == 1)
    def _():
        to_holder(0, 1).start()
        for oz in Z_ODD:
            for r in range(2):
                from_holder(oz, r)
        to_holder(0, 1).wait_send()

    for copy in copies:
        copy.wait_send()
    for i in range(OUT // 8):
        out_ref[i * 8 : i * 8 + 8, :] = fin[i]


def body(features, centers, labels, coeffs, precond):
    any_space = pl.BlockSpec(memory_space=pl.ANY)
    V = pltpu.VMEM
    dma = pltpu.SemaphoreType.DMA
    scratch = [
        V((ROWS, D), f32),
        V((2, CENT, D), f32),
        V((8, RS_ROWS), jnp.int32),
        V((OUT, CENT), f32),
        V((OUTS, CENT), f32),
        V((ROWS, 2 * D), bf16),
        V((ROWS, 2 * D), bf16),
        V((ROWS, 2 * D), bf16),
        V((CENT, 2 * D), bf16),
        V((CENT, 2 * D), bf16),
        V((8, ROWS), f32),
        V((2, CENT, ROWS), bf16),
        V((2, CENT, ROWS), bf16),
        V((2, PROWS, CENT), f32),
        V((2, PROWS, CENT), bf16),
        V((2, PROWS, CENT), bf16),
        V((X, OUTS, RS_ROWS), f32),
        V((X, OUTS, RS_ROWS), f32),
        V((X, OUTS, RS_ROWS), f32),
        V((2, OUTS, CENT), f32),
        V((X, OUTS, RS_PROWS), f32),
        V((2, OUTS, CENT), f32),
        V((CHIPS, 8, RS_ROWS), f32),
        V((CHIPS, 8, RS_ROWS), f32),
        V((CHIPS, 8, RS_ROWS), f32),
        V((Z, 8, CENT), f32),
        V((Z, 8, CENT), f32),
        V((Z, 8, CENT), f32),
        V((CHIPS, 8, RS_PROWS), f32),
        V((CHIPS, 8, RS_PROWS), f32),
        V((CHIPS, 8, RS_PROWS), f32),
        V((Z, 8, CENT + 128), f32),
        V((Z, 8, CENT + 128), f32),
        V((Z, 8, CENT), f32),
        V((STEPS, 8, 128), f32),
        V((STEPS, Z, 8, 128), f32),
        V((OUT // 8, 8, CENT), f32),
        dma((5,)),
        dma((9,)),
        dma((9,)),
        dma((8,)),
        dma((8,)),
    ]
    for count in (CHIPS, CHIPS, Z, Z, CHIPS, CHIPS, Z, Z):
        scratch += [dma((count,)), dma((count,))]
    scratch += [dma((STEPS, Z)), dma((STEPS, Z)), dma((Z,)), dma((2 * Z,))]
    out = pl.pallas_call(
        kernel,
        out_shape=pltpu.VMEM((OUT, CENT), f32),
        in_specs=[any_space] * 5,
        out_specs=pl.BlockSpec(memory_space=pltpu.VMEM),
        scratch_shapes=scratch,
        compiler_params=pltpu.CompilerParams(
            collective_id=0, has_side_effects=True, vmem_limit_bytes=60 * 1024 * 1024
        ),
        name="falkon",
    )(features, centers, labels.T, coeffs.T, precond)
    return out.T


def solution(mesh):
    in_specs = (
        P("rows", None),
        P("centers", None),
        P("rows", None),
        P("centers", None),
        P("rows", "centers"),
    )
    return jax.shard_map(body, mesh=mesh, in_specs=in_specs, out_specs=P("centers", None), check_vma=False)
```

```python
import functools

import jax
import jax.numpy as jnp
from jax import lax
from jax.experimental import pallas as pl
from jax.experimental.pallas import tpu as pltpu
from jax.sharding import PartitionSpec as P

STEPS = 2
step_size = 0.5
epsilon = 1e-06
LOG2E = 1.4426950408889634

Z, Y, X = 8, 4, 4
CHIPS = Y * X
D = 128
OUT = 64
OUTS = OUT // 2
GROUPS = OUTS // 8
ROWS = 1024
CENT = 512
PROWS = 2048
RS_ROWS = ROWS // X
RS_PROWS = PROWS // X
FAR_FIRST = (2, 1, 3, 0)
NEAR_FIRST = (0, 1, 3, 2)
Z_FAR = (4, 3, 5, 2, 6, 1, 7)
PLANE_FAR = (
    (2, 2), (1, 2), (2, 1), (3, 2), (2, 3), (1, 1), (3, 3), (1, 3), (3, 1), (2, 0), (0, 2), (1, 0), (0, 1), (3, 0), (0, 3),
)
PAIRS = Z // 2
PAIR = 2 * CENT // PAIRS
PIECE = PAIR // 2
f32 = jnp.float32
bf16 = jnp.bfloat16
MESH = pl.DeviceIdType.MESH


def split(x):
    hi = x.astype(bf16)
    lo = (x - hi.astype(f32)).astype(bf16)
    return hi, lo


def split3(x):
    hi = x.astype(bf16)
    rest = x - hi.astype(f32)
    mid = rest.astype(bf16)
    lo = (rest - mid.astype(f32)).astype(bf16)
    return hi, mid, lo


def stacked(x):
    hi, lo = split(x)
    return jnp.concatenate([hi, lo], axis=0), hi


def dot(a, b, contract):
    return lax.dot_general(a, b, (((1,), (contract,)), ((), ())), preferred_element_type=f32)


def product(lhs, w_hi, w_lo, contract):
    both, hi = lhs
    n = hi.shape[0]
    r = dot(both, w_hi, contract)
    s = dot(hi, w_lo, contract)
    return r[:n] + r[n:] + s


def kernel(
    feat_hbm, cent_hbm, lab_hbm, coef_hbm, prec_hbm, out_ref,
    feat, cent, lab, coef, coef_pair, r1, r2, r3, l1, l2, norm, k_hi, k_lo, p_raw, p_hi, p_lo,
    pair_s, pair_r, log_a, col_a, fwd_a,
    log_p, log_r, res_f, gra_p, gra_r, gra_f, fwd_p, fwd_r, fwd_f, bak_p, bak_r, a_f, sq_s, sq_r, fin,
    load_sem, pair_send, pair_recv, pch_send, pch_recv,
    log_ss, log_rs, res_ss, res_rs, gra_ss, gra_rs, grf_ss, grf_rs,
    fwd_ss, fwd_rs, fwf_ss, fwf_rs, bak_ss, bak_rs, af_ss, af_rs, sq_ss, sq_rs, fin_ss, fin_rs,
):
    z = lax.axis_index("rows")
    c = lax.axis_index("centers")
    j = c // 2
    k = c % 2
    y = j // X
    x = j % X
    zp = z // 2
    zlo = z % 2
    other = 1 - k
    partner = c + 1 - 2 * k
    mine = pl.multiple_of(k * OUTS, OUTS)
    theirs = pl.multiple_of(other * OUTS, OUTS)

    lab_at = (
        pl.ds(pl.multiple_of(k * OUTS + y * 8, 8), 8),
        pl.ds(pl.multiple_of(x * RS_ROWS, RS_ROWS), RS_ROWS),
    )
    loads = [
        pltpu.make_async_copy(feat_hbm, feat, load_sem.at[0]),
        pltpu.make_async_copy(cent_hbm, cent.at[k], load_sem.at[1]),
        pltpu.make_async_copy(coef_hbm, coef, load_sem.at[2]),
        pltpu.make_async_copy(lab_hbm.at[lab_at], lab, load_sem.at[3]),
        pltpu.make_async_copy(prec_hbm, p_raw.at[k], load_sem.at[4]),
    ]
    for copy in loads:
        copy.start()

    barrier = pltpu.get_barrier_semaphore()
    pl.semaphore_signal(barrier, inc=1, device_id=(z, partner), device_id_type=MESH)

    def chip_at(dy, dx):
        return lax.rem(y + dy, Y) * X + lax.rem(x + dx, X)

    plane = PLANE_FAR
    for dy, dx in plane:
        pl.semaphore_signal(barrier, inc=1, device_id=(z, 2 * chip_at(dy, dx) + k), device_id_type=MESH)
    for oz in Z_FAR:
        pl.semaphore_signal(barrier, inc=1, device_id=(lax.rem(z + oz, Z), c), device_id_type=MESH)
        pl.semaphore_signal(barrier, inc=1, device_id=(lax.rem(z + oz, Z), partner), device_id_type=MESH)

    def remote(src, dst, send, recv, device):
        return pltpu.make_async_remote_copy(
            src_ref=src, dst_ref=dst, send_sem=send, recv_sem=recv, device_id=device, device_id_type=MESH
        )

    def to_pair(src, dst, n):
        return remote(src, dst, pair_send.at[n], pair_recv.at[n], (z, partner))

    def to_plane(src, dst, ss, rs, dy, dx):
        o = dy * X + dx
        return remote(src, dst, ss.at[o], rs.at[o], (z, 2 * chip_at(dy, dx) + k))

    def to_z(src, dst, ss, rs, oz):
        return remote(src, dst, ss.at[oz], rs.at[oz], (lax.rem(z + oz, Z), c))

    factor = 2.0 * LOG2E / D
    loads[0].wait()
    fx = feat[...]
    hi, mid, lo = split3(fx)
    r1[...] = jnp.concatenate([hi, hi], axis=1)
    r2[...] = jnp.concatenate([mid, mid], axis=1)
    r3[...] = jnp.concatenate([lo, hi], axis=1)
    hi, mid, lo = split3(fx * fx)
    ones = jnp.ones((16, D), bf16)
    row_norm = dot(ones, hi, 1) + dot(ones, mid, 1) + dot(ones, lo, 1)
    norm[...] = row_norm[:8] * factor

    def kernel_half(h):
        cx = cent[h]
        hi, mid, lo = split3(cx)
        l1[...] = jnp.concatenate([hi, mid], axis=1)
        l2[...] = jnp.concatenate([hi, lo], axis=1)
        cn = jnp.sum(cx * cx, axis=1, keepdims=True) * factor

        @pl.loop(0, X)
        def _(i):
            at = pl.ds(pl.multiple_of(i * RS_ROWS, RS_ROWS), RS_ROWS)
            cross = dot(l1[...], r1[at, :], 1) + dot(l1[...], r2[at, :], 1) + dot(l2[...], r3[at, :], 1)
            tile = jnp.exp2(cross * (2.0 * factor) - (cn + norm[:1, at]))
            hi, lo = split(tile)
            k_hi[h, :, at] = hi
            k_lo[h, :, at] = lo

    def precond_half(h):
        @pl.loop(0, PROWS // 128)
        def _(i):
            at = pl.multiple_of(i * 128, 128)
            hi, lo = split(p_raw[h, pl.ds(at, 128), :])
            p_hi[h, pl.ds(at, 128), :] = hi
            p_lo[h, pl.ds(at, 128), :] = lo

    precond_chunks = [
        remote(
            p_raw.at[k, pl.ds(i * 256, 256), :], p_raw.at[k, pl.ds(i * 256, 256), :],
            pch_send.at[i], pch_recv.at[i], (z, partner),
        )
        for i in range(8)
    ]

    loads[1].wait()
    kernel_half(k)
    loads[2].wait()

    def line_of(pieces, rg):
        return jnp.concatenate([pieces[og * X + rg] for og in range(GROUPS)], axis=0)

    def pair_of(pieces, p):
        return jnp.concatenate([pieces[2 * p], pieces[2 * p + 1]], axis=1)

    def pair_at(p):
        return p // 2, pl.ds(pl.multiple_of((p % 2) * PAIR, PAIR), PAIR)

    def row_block(dx, size):
        rg = lax.rem(x + dx, X)
        return rg, pl.ds(pl.multiple_of(rg * size, size), size)

    def scatter_plane(pieces, landing, ss, rs, dx):
        for dy in FAR_FIRST:
            if (dy, dx) != (0, 0):
                to_plane(pieces.at[chip_at(dy, dx)], landing.at[dy * X + dx], ss, rs, dy, dx).start()

    def plane_sum(pieces, landing, ss, rs):
        total = pieces[j]
        for dy, dx in reversed(plane):
            to_plane(pieces.at[j], landing.at[dy * X + dx], ss, rs, dy, dx).wait_recv()
            total = total + landing[dy * X + dx]
        return total

    def gather_plane(pieces, ss, rs):
        for dy, dx in plane:
            to_plane(pieces.at[j], pieces.at[j], ss, rs, dy, dx).start()

    def arrived_line(pieces, ss, rs, dx):
        for dy in reversed(FAR_FIRST):
            if (dy, dx) != (0, 0):
                to_plane(pieces.at[j], pieces.at[chip_at(Y - dy, X - dx)], ss, rs, dy, dx).wait_recv()

    def sent_plane(pieces, ss, rs):
        for dy, dx in plane:
            to_plane(pieces.at[j], pieces.at[j], ss, rs, dy, dx).wait_send()

    def pair_members(r):
        p = lax.rem(zp + r, PAIRS)
        return p, ([2 * p, 2 * p + 1] if r else [z + 1 - 2 * zlo])

    def scatter_z(pieces, landing, ss, rs, r):
        for other_z in pair_members(r)[1]:
            oz = lax.rem(other_z - z + Z, Z)
            to_z(pieces.at[other_z], landing.at[oz], ss, rs, oz).start()

    def z_sum(pieces, landing, ss, rs):
        total = pieces[z]
        for oz in reversed(Z_FAR):
            to_z(pieces.at[z], landing.at[oz], ss, rs, oz).wait_recv()
            total = total + landing[oz]
        return total

    def gather_z(pieces, ss, rs):
        for oz in Z_FAR:
            to_z(pieces.at[z], pieces.at[z], ss, rs, oz).start()

    def arrived_pair(pieces, ss, rs, r):
        for other_z in pair_members(r)[1]:
            to_z(pieces.at[z], pieces.at[other_z], ss, rs, lax.rem(z - other_z + Z, Z)).wait_recv()

    def sent_z(pieces, ss, rs):
        for oz in Z_FAR:
            to_z(pieces.at[z], pieces.at[z], ss, rs, oz).wait_send()

    def send_logits(dx, part):
        rg = lax.rem(x + dx, X)
        for og in range(GROUPS):
            log_p[og * X + rg] = part[og * 8 : og * 8 + 8]
        scatter_plane(log_p, log_r, log_ss, log_rs, dx)

    lhs = stacked(jnp.concatenate([coef[pl.ds(theirs, OUTS), :], coef[pl.ds(mine, OUTS), :]], axis=0))
    for n, dx in enumerate(FAR_FIRST):
        rg, at = row_block(dx, RS_ROWS)
        part = product(lhs, k_hi[k, :, at], k_lo[k, :, at], 0)
        pair_s[n] = part[:OUTS]
        log_a[n] = part[OUTS:]
    pl.semaphore_wait(barrier, 1 + len(plane) + 2 * (Z - 1))
    pairs = [to_pair(pair_s.at[n], pair_r.at[n], n) for n in range(X)]
    for copy in pairs:
        copy.start()
    cent_pair = to_pair(cent.at[k], cent.at[k], 4)
    cent_pair.start()
    coef_copy = to_pair(coef.at[pl.ds(theirs, OUTS), :], coef_pair, 5)
    coef_copy.start()
    for n, dx in enumerate(FAR_FIRST):
        pairs[n].wait_recv()
        send_logits(dx, log_a[n] + pair_r[n])
    loads[4].wait()
    for copy in precond_chunks[:4]:
        copy.start()
    for copy in pairs:
        copy.wait_send()
    cent_pair.wait()
    kernel_half(other)
    coef_copy.wait()
    for i in range(CENT // PIECE):
        col = slice(i * PIECE, i * PIECE + PIECE)
        a_f[k * (Z // 2) + i] = coef[pl.ds(mine, OUTS), col]
        a_f[other * (Z // 2) + i] = coef_pair[:, col]
    precond_half(k)
    loads[3].wait()

    @pl.loop(0, STEPS)
    def _(step):
        total = plane_sum(log_p, log_r, log_ss, log_rs)
        res_f[j] = (jax.nn.sigmoid(total) - lab[...].astype(f32)) * (1.0 / (ROWS * Z))
        gather_plane(res_f, res_ss, res_rs)

        @pl.when(step == 0)
        def _():
            for copy in precond_chunks[4:]:
                copy.start()

        sent_plane(log_p, log_ss, log_rs)

        for dx in NEAR_FIRST:
            arrived_line(res_f, res_ss, res_rs, dx)
            rg, rows = row_block(X - dx, RS_ROWS)
            lhs = stacked(line_of(res_f, rg))
            for n, r in enumerate(FAR_FIRST):
                p = lax.rem(zp + r, PAIRS)
                h, at = pair_at(p)
                part = product(lhs, k_hi[h, at, rows], k_lo[h, at, rows], 1)
                if dx != NEAR_FIRST[0]:
                    part = col_a[n] + part
                if dx != NEAR_FIRST[-1]:
                    col_a[n] = part
                else:
                    gra_p[2 * p] = part[:, :PIECE]
                    gra_p[2 * p + 1] = part[:, PIECE:]
                    scatter_z(gra_p, gra_r, gra_ss, gra_rs, r)
        sent_plane(res_f, res_ss, res_rs)

        @pl.when(step == 0)
        def _():
            for copy in precond_chunks:
                copy.wait()
            precond_half(other)

        gra_f[z] = z_sum(gra_p, gra_r, gra_ss, gra_rs)
        gather_z(gra_f, grf_ss, grf_rs)
        sent_z(gra_p, gra_ss, gra_rs)

        for r in NEAR_FIRST:
            arrived_pair(gra_f, grf_ss, grf_rs, r)
            p = lax.rem(zp + r, PAIRS)
            h, at = pair_at(p)
            lhs = stacked(pair_of(gra_f, p))
            for n, dx in enumerate(FAR_FIRST):
                rg, rows = row_block(dx, RS_PROWS)
                part = product(lhs, p_hi[h, rows, at], p_lo[h, rows, at], 1)
                if r != NEAR_FIRST[0]:
                    part = fwd_a[n] + part
                if r != NEAR_FIRST[-1]:
                    fwd_a[n] = part
                else:
                    for og in range(GROUPS):
                        fwd_p[og * X + rg] = part[og * 8 : og * 8 + 8]
                    scatter_plane(fwd_p, fwd_r, fwd_ss, fwd_rs, dx)
        sent_z(gra_f, grf_ss, grf_rs)
        fwd_f[j] = plane_sum(fwd_p, fwd_r, fwd_ss, fwd_rs)
        gather_plane(fwd_f, fwf_ss, fwf_rs)
        sent_plane(fwd_p, fwd_ss, fwd_rs)

        def to_other_core(oz):
            return remote(
                sq_s.at[step], sq_r.at[step, oz], sq_ss.at[step, oz], sq_rs.at[step, oz],
                (lax.rem(z + oz, Z), partner),
            )

        square = jnp.zeros((8, 128), f32)
        for dx in NEAR_FIRST:
            arrived_line(fwd_f, fwf_ss, fwf_rs, dx)
            rg, rows = row_block(X - dx, RS_PROWS)
            line = line_of(fwd_f, rg)
            for og in range(GROUPS):
                for t in range(RS_PROWS // 128):
                    tile = line[og * 8 : og * 8 + 8, t * 128 : t * 128 + 128]
                    square = square + tile * tile
            if dx == NEAR_FIRST[-1]:
                sq_s[step] = square
                for i in range(Z):
                    bak_p[i, OUTS:] = square
                for oz in Z_FAR + (0,):
                    to_other_core(oz).start()
            lhs = stacked(line)
            for n, r in enumerate(FAR_FIRST):
                p = lax.rem(zp + r, PAIRS)
                h, at = pair_at(p)
                part = product(lhs, p_hi[h, rows, at], p_lo[h, rows, at], 0)
                if dx != NEAR_FIRST[0]:
                    part = col_a[n] + part
                if dx != NEAR_FIRST[-1]:
                    col_a[n] = part
                else:
                    bak_p[2 * p, :OUTS] = part[:, :PIECE]
                    bak_p[2 * p + 1, :OUTS] = part[:, PIECE:]
                    scatter_z(bak_p, bak_r, bak_ss, bak_rs, r)
        sent_plane(fwd_f, fwf_ss, fwf_rs)
        total = z_sum(bak_p, bak_r, bak_ss, bak_rs)
        square = total[OUTS:]
        for oz in range(Z):
            to_other_core(oz).wait_recv()
            square = square + sq_r[step, oz]
        square = jnp.sum(jnp.sum(square, axis=1, keepdims=True), axis=0, keepdims=True)
        scale = step_size / jnp.sqrt(square / (CENT * 2 * CHIPS * OUT) + epsilon)
        a_f[z] = a_f[z] - scale * total[:OUTS]

        @pl.when(step < STEPS - 1)
        def _():
            gather_z(a_f, af_ss, af_rs)

        sent_z(bak_p, bak_ss, bak_rs)
        for oz in range(Z):
            to_other_core(oz).wait_send()

        @pl.when(step < STEPS - 1)
        def _():
            for r in NEAR_FIRST:
                arrived_pair(a_f, af_ss, af_rs, r)
                p = lax.rem(zp + r, PAIRS)
                h, at = pair_at(p)
                lhs = stacked(pair_of(a_f, p))
                for n, dx in enumerate(FAR_FIRST):
                    rg, rows = row_block(dx, RS_ROWS)
                    part = product(lhs, k_hi[h, at, rows], k_lo[h, at, rows], 0)
                    if r != NEAR_FIRST[0]:
                        part = log_a[n] + part
                    if r != NEAR_FIRST[-1]:
                        log_a[n] = part
                    else:
                        send_logits(dx, part)
            sent_z(a_f, af_ss, af_rs)

    holder = z // (Z // 2)
    rel = lax.rem(k + holder, 2)

    def to_holder(oz, r):
        return remote(
            a_f.at[z], fin.at[k * (Z // 2) + lax.rem(z, Z // 2)], fin_ss.at[oz], fin_rs.at[oz * 2 + r],
            (lax.rem(z + oz, Z), 2 * j + holder),
        )

    copies = [to_holder(oz, rel) for oz in Z_FAR]
    for copy in copies:
        copy.start()

    @pl.when(rel == 0)
    def _():
        fin[k * (Z // 2) + lax.rem(z, Z // 2)] = a_f[z]

    @pl.when(rel == 1)
    def _():
        to_holder(0, 1).start()
        to_holder(0, 1).wait_send()

    for i in range(Z // 2):
        source = k * (Z // 2) + i
        oz = lax.rem(z - source + Z, Z)

        def arrived(r):
            owner = k + r * (1 - 2 * k)
            remote(
                a_f.at[z], fin.at[owner * (Z // 2) + i], fin_ss.at[oz], fin_rs.at[oz * 2 + r], (z, partner)
            ).wait_recv()

        pl.when(source != z)(functools.partial(arrived, 0))
        arrived(1)
    for copy in copies:
        copy.wait_send()
    for n in range(2):
        for i in range(Z // 2):
            out_ref[n * OUTS : n * OUTS + OUTS, i * PIECE : i * PIECE + PIECE] = fin[n * (Z // 2) + i]


def body(features, centers, labels, coeffs, precond):
    any_space = pl.BlockSpec(memory_space=pl.ANY)
    V = pltpu.VMEM
    dma = pltpu.SemaphoreType.DMA
    scratch = [
        V((ROWS, D), f32),
        V((2, CENT, D), f32),
        V((8, RS_ROWS), jnp.int32),
        V((OUT, CENT), f32),
        V((OUTS, CENT), f32),
        V((ROWS, 2 * D), bf16),
        V((ROWS, 2 * D), bf16),
        V((ROWS, 2 * D), bf16),
        V((CENT, 2 * D), bf16),
        V((CENT, 2 * D), bf16),
        V((8, ROWS), f32),
        V((2, CENT, ROWS), bf16),
        V((2, CENT, ROWS), bf16),
        V((2, PROWS, CENT), f32),
        V((2, PROWS, CENT), bf16),
        V((2, PROWS, CENT), bf16),
        V((X, OUTS, RS_ROWS), f32),
        V((X, OUTS, RS_ROWS), f32),
        V((X, OUTS, RS_ROWS), f32),
        V((PAIRS, OUTS, PAIR), f32),
        V((X, OUTS, RS_PROWS), f32),
        V((CHIPS, 8, RS_ROWS), f32),
        V((CHIPS, 8, RS_ROWS), f32),
        V((CHIPS, 8, RS_ROWS), f32),
        V((Z, OUTS, PIECE), f32),
        V((Z, OUTS, PIECE), f32),
        V((Z, OUTS, PIECE), f32),
        V((CHIPS, 8, RS_PROWS), f32),
        V((CHIPS, 8, RS_PROWS), f32),
        V((CHIPS, 8, RS_PROWS), f32),
        V((Z, OUTS + 8, PIECE), f32),
        V((Z, OUTS + 8, PIECE), f32),
        V((Z, OUTS, PIECE), f32),
        V((STEPS, 8, 128), f32),
        V((STEPS, Z, 8, 128), f32),
        V((Z, OUTS, PIECE), f32),
        dma((5,)),
        dma((9,)),
        dma((9,)),
        dma((8,)),
        dma((8,)),
    ]
    for count in (CHIPS, CHIPS, Z, Z, CHIPS, CHIPS, Z, Z):
        scratch += [dma((count,)), dma((count,))]
    scratch += [dma((STEPS, Z)), dma((STEPS, Z)), dma((Z,)), dma((2 * Z,))]
    out = pl.pallas_call(
        kernel,
        out_shape=pltpu.VMEM((OUT, CENT), f32),
        in_specs=[any_space] * 5,
        out_specs=pl.BlockSpec(memory_space=pltpu.VMEM),
        scratch_shapes=scratch,
        compiler_params=pltpu.CompilerParams(
            collective_id=0, has_side_effects=True, vmem_limit_bytes=60 * 1024 * 1024
        ),
        name="falkon",
    )(features, centers, labels.T, coeffs.T, precond)
    return out.T


def solution(mesh):
    in_specs = (
        P("rows", None),
        P("centers", None),
        P("rows", None),
        P("centers", None),
        P("rows", "centers"),
    )
    return jax.shard_map(body, mesh=mesh, in_specs=in_specs, out_specs=P("centers", None), check_vma=False)
```

```python
import functools

import jax
import jax.numpy as jnp
from jax import lax
from jax.experimental import pallas as pl
from jax.experimental.pallas import tpu as pltpu
from jax.sharding import PartitionSpec as P

STEPS = 2
step_size = 0.5
epsilon = 1e-06
LOG2E = 1.4426950408889634

Z, Y, X = 8, 4, 4
CHIPS = Y * X
D = 128
OUT = 64
OUTS = OUT // 2
GROUPS = OUTS // 8
ROWS = 1024
CENT = 512
PROWS = 2048
RS_ROWS = ROWS // X
RS_PROWS = PROWS // X
FAR_FIRST = (2, 1, 3, 0)
NEAR_FIRST = (0, 1, 3, 2)
Z_FAR = (4, 3, 5, 2, 6, 1, 7)
PLANE_FAR = (
    (2, 2), (1, 2), (2, 1), (3, 2), (2, 3), (1, 1), (3, 3), (1, 3), (3, 1), (2, 0), (0, 2), (1, 0), (0, 1), (3, 0), (0, 3),
)
RING = tuple((oz, r) for oz in Z_FAR for r in range(2)) + ((0, 1),)
PAIRS = Z // 2
PAIR = 2 * CENT // PAIRS
PIECE = PAIR // 2
f32 = jnp.float32
bf16 = jnp.bfloat16
MESH = pl.DeviceIdType.MESH


def split(x):
    hi = x.astype(bf16)
    lo = (x - hi.astype(f32)).astype(bf16)
    return hi, lo


def split3(x):
    hi = x.astype(bf16)
    rest = x - hi.astype(f32)
    mid = rest.astype(bf16)
    lo = (rest - mid.astype(f32)).astype(bf16)
    return hi, mid, lo


def stacked(x):
    hi, lo = split(x)
    return jnp.concatenate([hi, lo], axis=0), hi


def dot(a, b, contract):
    return lax.dot_general(a, b, (((1,), (contract,)), ((), ())), preferred_element_type=f32)


def product(lhs, w_hi, w_lo, contract):
    both, hi = lhs
    n = hi.shape[0]
    r = dot(both, w_hi, contract)
    s = dot(hi, w_lo, contract)
    return r[:n] + r[n:] + s


def kernel(
    feat_hbm, cent_hbm, lab_hbm, coef_hbm, prec_hbm, out_ref,
    feat, cent, lab, coef, coef_pair, r1, r2, r3, l1, l2, norm, k_hi, k_lo, kt_hi, kt_lo, p_raw, p_hi, p_lo, pt_hi, pt_lo,
    pair_s, pair_r, log_a, col_a, fwd_a,
    log_p, log_r, res_f, gra_p, gra_r, gra_f, fwd_p, fwd_r, fwd_f, bak_p, bak_r, a_f, sq_s, sq_r, fin,
    load_sem, pair_send, pair_recv, pch_send, pch_recv,
    log_ss, log_rs, res_ss, res_rs, gra_ss, gra_rs, grf_ss, grf_rs,
    fwd_ss, fwd_rs, fwf_ss, fwf_rs, bak_ss, bak_rs, af_ss, af_rs, sq_ss, sq_rs, fin_ss, fin_rs,
):
    z = lax.axis_index("rows")
    c = lax.axis_index("centers")
    j = c // 2
    k = c % 2
    y = j // X
    x = j % X
    zp = z // 2
    zlo = z % 2
    other = 1 - k
    partner = c + 1 - 2 * k
    mine = pl.multiple_of(k * OUTS, OUTS)
    theirs = pl.multiple_of(other * OUTS, OUTS)

    def chip_at(dy, dx):
        return lax.rem(y + dy, Y) * X + lax.rem(x + dx, X)

    barrier = pltpu.get_barrier_semaphore()

    def greet(device):
        pl.semaphore_signal(barrier, inc=1, device_id=device, device_id_type=MESH)

    plane = PLANE_FAR
    for n, (dy, dx) in enumerate(plane):
        greet((z, 2 * chip_at(dy, dx) + k))
        if n < len(Z_FAR):
            oz = lax.rem(z + Z_FAR[n], Z)
            greet((oz, c))
            greet((oz, partner))
    greet((z, partner))

    lab_at = (
        pl.ds(pl.multiple_of(k * OUTS + y * 8, 8), 8),
        pl.ds(pl.multiple_of(x * RS_ROWS, RS_ROWS), RS_ROWS),
    )
    loads = [
        pltpu.make_async_copy(feat_hbm, feat, load_sem.at[0]),
        pltpu.make_async_copy(cent_hbm, cent.at[k], load_sem.at[1]),
        pltpu.make_async_copy(coef_hbm, coef, load_sem.at[2]),
        pltpu.make_async_copy(lab_hbm.at[lab_at], lab, load_sem.at[3]),
        pltpu.make_async_copy(prec_hbm, p_raw.at[k], load_sem.at[4]),
    ]
    for copy in loads:
        copy.start()

    def remote(src, dst, send, recv, device):
        return pltpu.make_async_remote_copy(
            src_ref=src, dst_ref=dst, send_sem=send, recv_sem=recv, device_id=device, device_id_type=MESH
        )

    def to_pair(src, dst, n):
        return remote(src, dst, pair_send.at[n], pair_recv.at[n], (z, partner))

    def to_plane(src, dst, ss, rs, dy, dx):
        o = dy * X + dx
        return remote(src, dst, ss.at[o], rs.at[o], (z, 2 * chip_at(dy, dx) + k))

    def to_z(src, dst, ss, rs, oz):
        return remote(src, dst, ss.at[oz], rs.at[oz], (lax.rem(z + oz, Z), c))

    factor = 2.0 * LOG2E / D
    loads[0].wait()
    fx = feat[...]
    hi, mid, lo = split3(fx)
    r1[...] = jnp.concatenate([hi, hi], axis=1)
    r2[...] = jnp.concatenate([mid, mid], axis=1)
    r3[...] = jnp.concatenate([lo, hi], axis=1)
    hi, mid, lo = split3(fx * fx)
    ones = jnp.ones((16, D), bf16)
    row_norm = dot(ones, hi, 1) + dot(ones, mid, 1) + dot(ones, lo, 1)
    norm[...] = row_norm[:8] * factor

    def kernel_half(h):
        cx = cent[h]
        hi, mid, lo = split3(cx)
        l1[...] = jnp.concatenate([hi, mid], axis=1)
        l2[...] = jnp.concatenate([hi, lo], axis=1)
        cn = jnp.sum(cx * cx, axis=1, keepdims=True) * factor

        @pl.loop(0, X)
        def _(i):
            at = pl.ds(pl.multiple_of(i * RS_ROWS, RS_ROWS), RS_ROWS)
            cross = dot(l1[...], r1[at, :], 1) + dot(l1[...], r2[at, :], 1) + dot(l2[...], r3[at, :], 1)
            tile = jnp.exp2(cross * (2.0 * factor) - (cn + norm[:1, at]))
            hi, lo = split(tile)
            k_hi[h, :, at] = hi
            k_lo[h, :, at] = lo
            hi, lo = split(tile.T)
            kt_hi[h, at, :] = hi
            kt_lo[h, at, :] = lo

    def precond_half(h):
        @pl.loop(0, PROWS // 128)
        def _(i):
            at = pl.multiple_of(i * 128, 128)
            tile = p_raw[h, pl.ds(at, 128), :]
            hi, lo = split(tile)
            p_hi[h, pl.ds(at, 128), :] = hi
            p_lo[h, pl.ds(at, 128), :] = lo
            hi, lo = split(tile.T)
            pt_hi[h, :, pl.ds(at, 128)] = hi
            pt_lo[h, :, pl.ds(at, 128)] = lo

    precond_chunks = [
        remote(
            p_raw.at[k, pl.ds(i * 256, 256), :], p_raw.at[k, pl.ds(i * 256, 256), :],
            pch_send.at[i], pch_recv.at[i], (z, partner),
        )
        for i in range(8)
    ]

    loads[1].wait()
    kernel_half(k)
    loads[2].wait()

    def line_of(pieces, rg):
        return jnp.concatenate([pieces[og * X + rg] for og in range(GROUPS)], axis=0)

    def pair_of(pieces, p):
        return jnp.concatenate([pieces[2 * p], pieces[2 * p + 1]], axis=1)

    def pair_at(p):
        return p // 2, pl.ds(pl.multiple_of((p % 2) * PAIR, PAIR), PAIR)

    def row_block(dx, size):
        rg = lax.rem(x + dx, X)
        return rg, pl.ds(pl.multiple_of(rg * size, size), size)

    def scatter_plane(pieces, landing, ss, rs, dx):
        for dy in FAR_FIRST:
            if (dy, dx) != (0, 0):
                to_plane(pieces.at[chip_at(dy, dx)], landing.at[dy * X + dx], ss, rs, dy, dx).start()

    def plane_sum(pieces, landing, ss, rs):
        total = pieces[j]
        for dy, dx in reversed(plane):
            to_plane(pieces.at[j], landing.at[dy * X + dx], ss, rs, dy, dx).wait_recv()
            total = total + landing[dy * X + dx]
        return total

    def gather_plane(pieces, ss, rs):
        for dy, dx in plane:
            to_plane(pieces.at[j], pieces.at[j], ss, rs, dy, dx).start()

    def arrived_line(pieces, ss, rs, dx):
        for dy in reversed(FAR_FIRST):
            if (dy, dx) != (0, 0):
                to_plane(pieces.at[j], pieces.at[chip_at(Y - dy, X - dx)], ss, rs, dy, dx).wait_recv()

    def sent_plane(pieces, ss, rs):
        for dy, dx in plane:
            to_plane(pieces.at[j], pieces.at[j], ss, rs, dy, dx).wait_send()

    def pair_members(r):
        p = lax.rem(zp + r, PAIRS)
        return p, ([2 * p, 2 * p + 1] if r else [z + 1 - 2 * zlo])

    def scatter_z(pieces, landing, ss, rs, r):
        for other_z in pair_members(r)[1]:
            oz = lax.rem(other_z - z + Z, Z)
            to_z(pieces.at[other_z], landing.at[oz], ss, rs, oz).start()

    def z_sum(pieces, landing, ss, rs):
        total = pieces[z]
        for oz in reversed(Z_FAR):
            to_z(pieces.at[z], landing.at[oz], ss, rs, oz).wait_recv()
            total = total + landing[oz]
        return total

    def gather_z(pieces, ss, rs):
        for oz in Z_FAR:
            to_z(pieces.at[z], pieces.at[z], ss, rs, oz).start()

    def arrived_pair(pieces, ss, rs, r):
        for other_z in pair_members(r)[1]:
            to_z(pieces.at[z], pieces.at[other_z], ss, rs, lax.rem(z - other_z + Z, Z)).wait_recv()

    def sent_z(pieces, ss, rs):
        for oz in Z_FAR:
            to_z(pieces.at[z], pieces.at[z], ss, rs, oz).wait_send()

    def send_logits(dx, part):
        rg = lax.rem(x + dx, X)
        for og in range(GROUPS):
            log_p[og * X + rg] = part[og * 8 : og * 8 + 8]
        scatter_plane(log_p, log_r, log_ss, log_rs, dx)

    lhs = stacked(jnp.concatenate([coef[pl.ds(theirs, OUTS), :], coef[pl.ds(mine, OUTS), :]], axis=0))
    for n, dx in enumerate(FAR_FIRST):
        rg, at = row_block(dx, RS_ROWS)
        part = product(lhs, k_hi[k, :, at], k_lo[k, :, at], 0)
        pair_s[n] = part[:OUTS]
        log_a[n] = part[OUTS:]
    pl.semaphore_wait(barrier, 1 + len(plane) + 2 * (Z - 1))
    pairs = [to_pair(pair_s.at[n], pair_r.at[n], n) for n in range(X)]
    for copy in pairs:
        copy.start()
    cent_pair = to_pair(cent.at[k], cent.at[k], 4)
    cent_pair.start()
    coef_copy = to_pair(coef.at[pl.ds(theirs, OUTS), :], coef_pair, 5)
    coef_copy.start()
    for n, dx in enumerate(FAR_FIRST):
        pairs[n].wait_recv()
        send_logits(dx, log_a[n] + pair_r[n])
    loads[4].wait()
    for copy in precond_chunks[:4]:
        copy.start()
    for copy in pairs:
        copy.wait_send()
    cent_pair.wait()
    kernel_half(other)
    coef_copy.wait()
    for i in range(CENT // PIECE):
        col = slice(i * PIECE, i * PIECE + PIECE)
        a_f[k * (Z // 2) + i] = coef[pl.ds(mine, OUTS), col]
        a_f[other * (Z // 2) + i] = coef_pair[:, col]
    precond_half(k)
    loads[3].wait()

    @pl.loop(0, STEPS)
    def _(step):
        total = plane_sum(log_p, log_r, log_ss, log_rs)
        res_f[j] = (jax.nn.sigmoid(total) - lab[...].astype(f32)) * (1.0 / (ROWS * Z))
        gather_plane(res_f, res_ss, res_rs)

        @pl.when(step == 0)
        def _():
            for copy in precond_chunks[4:]:
                copy.start()

        sent_plane(log_p, log_ss, log_rs)

        for dx in NEAR_FIRST:
            arrived_line(res_f, res_ss, res_rs, dx)
            rg, rows = row_block(X - dx, RS_ROWS)
            lhs = stacked(line_of(res_f, rg))
            for n, r in enumerate(FAR_FIRST):
                p = lax.rem(zp + r, PAIRS)
                h, at = pair_at(p)
                part = product(lhs, kt_hi[h, rows, at], kt_lo[h, rows, at], 0)
                if dx != NEAR_FIRST[0]:
                    part = col_a[n] + part
                if dx != NEAR_FIRST[-1]:
                    col_a[n] = part
                else:
                    gra_p[2 * p] = part[:, :PIECE]
                    gra_p[2 * p + 1] = part[:, PIECE:]
                    scatter_z(gra_p, gra_r, gra_ss, gra_rs, r)
        sent_plane(res_f, res_ss, res_rs)

        @pl.when(step == 0)
        def _():
            for copy in precond_chunks:
                copy.wait()
            precond_half(other)

        gra_f[z] = z_sum(gra_p, gra_r, gra_ss, gra_rs)
        gather_z(gra_f, grf_ss, grf_rs)
        sent_z(gra_p, gra_ss, gra_rs)

        for r in NEAR_FIRST:
            arrived_pair(gra_f, grf_ss, grf_rs, r)
            p = lax.rem(zp + r, PAIRS)
            h, at = pair_at(p)
            lhs = stacked(pair_of(gra_f, p))
            for n, dx in enumerate(FAR_FIRST):
                rg, rows = row_block(dx, RS_PROWS)
                part = product(lhs, pt_hi[h, at, rows], pt_lo[h, at, rows], 0)
                if r != NEAR_FIRST[0]:
                    part = fwd_a[n] + part
                if r != NEAR_FIRST[-1]:
                    fwd_a[n] = part
                else:
                    for og in range(GROUPS):
                        fwd_p[og * X + rg] = part[og * 8 : og * 8 + 8]
                    scatter_plane(fwd_p, fwd_r, fwd_ss, fwd_rs, dx)
        sent_z(gra_f, grf_ss, grf_rs)
        fwd_f[j] = plane_sum(fwd_p, fwd_r, fwd_ss, fwd_rs)
        gather_plane(fwd_f, fwf_ss, fwf_rs)
        sent_plane(fwd_p, fwd_ss, fwd_rs)

        def square_to(oz, r):
            n = oz * 2 + r
            return remote(
                sq_s.at[step], sq_r.at[step, n], sq_ss.at[step, n], sq_rs.at[step, n],
                (lax.rem(z + oz, Z), partner if r else c),
            )

        square = jnp.zeros((8, 128), f32)
        for dx in NEAR_FIRST:
            arrived_line(fwd_f, fwf_ss, fwf_rs, dx)
            rg, rows = row_block(X - dx, RS_PROWS)
            line = line_of(fwd_f, rg)
            for og in range(GROUPS):
                for t in range(RS_PROWS // 128):
                    tile = line[og * 8 : og * 8 + 8, t * 128 : t * 128 + 128]
                    square = square + tile * tile
            if dx == NEAR_FIRST[-1]:
                square = jnp.sum(square, axis=0, keepdims=True)
                sq_s[step] = square
                for oz, r in RING:
                    square_to(oz, r).start()
            lhs = stacked(line)
            for n, r in enumerate(FAR_FIRST):
                p = lax.rem(zp + r, PAIRS)
                h, at = pair_at(p)
                part = product(lhs, p_hi[h, rows, at], p_lo[h, rows, at], 0)
                if dx != NEAR_FIRST[0]:
                    part = col_a[n] + part
                if dx != NEAR_FIRST[-1]:
                    col_a[n] = part
                else:
                    bak_p[2 * p] = part[:, :PIECE]
                    bak_p[2 * p + 1] = part[:, PIECE:]
                    scatter_z(bak_p, bak_r, bak_ss, bak_rs, r)
        sent_plane(fwd_f, fwf_ss, fwf_rs)
        for oz, r in reversed(RING):
            square_to(oz, r).wait_recv()
            square = square + sq_r[step, oz * 2 + r]
        square = jnp.sum(square, axis=1, keepdims=True)
        scale = step_size / jnp.sqrt(square / (CENT * 2 * CHIPS * OUT) + epsilon)
        a_f[z] = a_f[z] - scale * z_sum(bak_p, bak_r, bak_ss, bak_rs)

        @pl.when(step < STEPS - 1)
        def _():
            gather_z(a_f, af_ss, af_rs)

        sent_z(bak_p, bak_ss, bak_rs)
        for oz, r in RING:
            square_to(oz, r).wait_send()

        @pl.when(step < STEPS - 1)
        def _():
            for r in NEAR_FIRST:
                arrived_pair(a_f, af_ss, af_rs, r)
                p = lax.rem(zp + r, PAIRS)
                h, at = pair_at(p)
                lhs = stacked(pair_of(a_f, p))
                for n, dx in enumerate(FAR_FIRST):
                    rg, rows = row_block(dx, RS_ROWS)
                    part = product(lhs, k_hi[h, at, rows], k_lo[h, at, rows], 0)
                    if r != NEAR_FIRST[0]:
                        part = log_a[n] + part
                    if r != NEAR_FIRST[-1]:
                        log_a[n] = part
                    else:
                        send_logits(dx, part)
            sent_z(a_f, af_ss, af_rs)

    holder = z // (Z // 2)
    rel = lax.rem(k + holder, 2)

    def to_holder(oz, r):
        return remote(
            a_f.at[z], fin.at[k * (Z // 2) + lax.rem(z, Z // 2)], fin_ss.at[oz], fin_rs.at[oz * 2 + r],
            (lax.rem(z + oz, Z), 2 * j + holder),
        )

    copies = [to_holder(oz, rel) for oz in Z_FAR]
    for copy in copies:
        copy.start()

    @pl.when(rel == 0)
    def _():
        fin[k * (Z // 2) + lax.rem(z, Z // 2)] = a_f[z]

    @pl.when(rel == 1)
    def _():
        to_holder(0, 1).start()
        to_holder(0, 1).wait_send()

    for i in range(Z // 2):
        source = k * (Z // 2) + i
        oz = lax.rem(z - source + Z, Z)

        def arrived(r):
            owner = k + r * (1 - 2 * k)
            remote(
                a_f.at[z], fin.at[owner * (Z // 2) + i], fin_ss.at[oz], fin_rs.at[oz * 2 + r], (z, partner)
            ).wait_recv()

        pl.when(source != z)(functools.partial(arrived, 0))
        arrived(1)
    for copy in copies:
        copy.wait_send()
    for n in range(2):
        for i in range(Z // 2):
            out_ref[n * OUTS : n * OUTS + OUTS, i * PIECE : i * PIECE + PIECE] = fin[n * (Z // 2) + i]


def body(features, centers, labels, coeffs, precond):
    any_space = pl.BlockSpec(memory_space=pl.ANY)
    V = pltpu.VMEM
    dma = pltpu.SemaphoreType.DMA
    scratch = [
        V((ROWS, D), f32),
        V((2, CENT, D), f32),
        V((8, RS_ROWS), jnp.int32),
        V((OUT, CENT), f32),
        V((OUTS, CENT), f32),
        V((ROWS, 2 * D), bf16),
        V((ROWS, 2 * D), bf16),
        V((ROWS, 2 * D), bf16),
        V((CENT, 2 * D), bf16),
        V((CENT, 2 * D), bf16),
        V((8, ROWS), f32),
        V((2, CENT, ROWS), bf16),
        V((2, CENT, ROWS), bf16),
        V((2, ROWS, CENT), bf16),
        V((2, ROWS, CENT), bf16),
        V((2, PROWS, CENT), f32),
        V((2, PROWS, CENT), bf16),
        V((2, PROWS, CENT), bf16),
        V((2, CENT, PROWS), bf16),
        V((2, CENT, PROWS), bf16),
        V((X, OUTS, RS_ROWS), f32),
        V((X, OUTS, RS_ROWS), f32),
        V((X, OUTS, RS_ROWS), f32),
        V((PAIRS, OUTS, PAIR), f32),
        V((X, OUTS, RS_PROWS), f32),
        V((CHIPS, 8, RS_ROWS), f32),
        V((CHIPS, 8, RS_ROWS), f32),
        V((CHIPS, 8, RS_ROWS), f32),
        V((Z, OUTS, PIECE), f32),
        V((Z, OUTS, PIECE), f32),
        V((Z, OUTS, PIECE), f32),
        V((CHIPS, 8, RS_PROWS), f32),
        V((CHIPS, 8, RS_PROWS), f32),
        V((CHIPS, 8, RS_PROWS), f32),
        V((Z, OUTS, PIECE), f32),
        V((Z, OUTS, PIECE), f32),
        V((Z, OUTS, PIECE), f32),
        V((STEPS, 1, 128), f32),
        V((STEPS, 2 * Z, 1, 128), f32),
        V((Z, OUTS, PIECE), f32),
        dma((5,)),
        dma((9,)),
        dma((9,)),
        dma((8,)),
        dma((8,)),
    ]
    for count in (CHIPS, CHIPS, Z, Z, CHIPS, CHIPS, Z, Z):
        scratch += [dma((count,)), dma((count,))]
    scratch += [dma((STEPS, 2 * Z)), dma((STEPS, 2 * Z)), dma((Z,)), dma((2 * Z,))]
    out = pl.pallas_call(
        kernel,
        out_shape=pltpu.VMEM((OUT, CENT), f32),
        in_specs=[any_space] * 5,
        out_specs=pl.BlockSpec(memory_space=pltpu.VMEM),
        scratch_shapes=scratch,
        compiler_params=pltpu.CompilerParams(
            collective_id=0, has_side_effects=True, vmem_limit_bytes=60 * 1024 * 1024
        ),
        name="falkon",
    )(features, centers, labels.T, coeffs.T, precond)
    return out.T


def solution(mesh):
    in_specs = (
        P("rows", None),
        P("centers", None),
        P("rows", None),
        P("centers", None),
        P("rows", "centers"),
    )
    return jax.shard_map(body, mesh=mesh, in_specs=in_specs, out_specs=P("centers", None), check_vma=False)
```

```python
import functools

import jax
import jax.numpy as jnp
from jax import lax
from jax.experimental import pallas as pl
from jax.experimental.pallas import tpu as pltpu
from jax.sharding import PartitionSpec as P

STEPS = 2
step_size = 0.5
epsilon = 1e-06
LOG2E = 1.4426950408889634

Z, Y, X = 8, 4, 4
CHIPS = Y * X
D = 128
OUT = 64
OUTS = OUT // 2
GROUPS = OUTS // 8
ROWS = 1024
CENT = 512
PROWS = 2048
RS_ROWS = ROWS // X
RS_PROWS = PROWS // X
FAR_FIRST = (2, 1, 3, 0)
NEAR_FIRST = (0, 1, 3, 2)
Z_FAR = (4, 3, 5, 2, 6, 1, 7)
PLANE_FAR = (
    (2, 2), (1, 2), (2, 1), (3, 2), (2, 3), (1, 1), (3, 3), (1, 3), (3, 1), (2, 0), (0, 2), (1, 0), (0, 1), (3, 0), (0, 3),
)
RING = tuple((oz, r) for oz in Z_FAR for r in range(2)) + ((0, 1),)
PAIRS = Z // 2
PAIR = 2 * CENT // PAIRS
PIECE = PAIR // 2
f32 = jnp.float32
bf16 = jnp.bfloat16
MESH = pl.DeviceIdType.MESH


def split(x):
    hi = x.astype(bf16)
    lo = (x - hi.astype(f32)).astype(bf16)
    return hi, lo


def split3(x):
    hi = x.astype(bf16)
    rest = x - hi.astype(f32)
    mid = rest.astype(bf16)
    lo = (rest - mid.astype(f32)).astype(bf16)
    return hi, mid, lo


def stacked(x):
    hi, lo = split(x)
    return jnp.concatenate([hi, lo], axis=0), hi


def dot(a, b, contract):
    return lax.dot_general(a, b, (((1,), (contract,)), ((), ())), preferred_element_type=f32)


def product(lhs, w_hi, w_lo, contract):
    both, hi = lhs
    n = hi.shape[0]
    r = dot(both, w_hi, contract)
    s = dot(hi, w_lo, contract)
    return r[:n] + r[n:] + s


def kernel(
    feat_hbm, cent_hbm, lab_hbm, coef_hbm, prec_hbm, out_ref,
    feat, cent, lab, coef, coef_pair, r1, r2, r3, l1, l2, norm, k_hi, k_lo, kt_hi, kt_lo, p_raw, p_hi, p_lo, pt_hi, pt_lo,
    pair_s, pair_r, log_a, col_a, fwd_a,
    log_p, log_r, res_f, gra_p, gra_r, gra_f, fwd_p, fwd_r, fwd_f, bak_p, bak_r, a_f, sq_s, sq_r, fin,
    load_sem, pair_send, pair_recv, pch_send, pch_recv,
    log_ss, log_rs, res_ss, res_rs, gra_ss, gra_rs, grf_ss, grf_rs,
    fwd_ss, fwd_rs, fwf_ss, fwf_rs, bak_ss, bak_rs, af_ss, af_rs, sq_ss, sq_rs, fin_ss, fin_rs,
):
    z = lax.axis_index("rows")
    c = lax.axis_index("centers")
    j = c // 2
    k = c % 2
    y = j // X
    x = j % X
    zp = z // 2
    zlo = z % 2
    other = 1 - k
    partner = c + 1 - 2 * k
    mine = pl.multiple_of(k * OUTS, OUTS)
    theirs = pl.multiple_of(other * OUTS, OUTS)

    def chip_at(dy, dx):
        return lax.rem(y + dy, Y) * X + lax.rem(x + dx, X)

    barrier = pltpu.get_barrier_semaphore()

    def greet(device):
        pl.semaphore_signal(barrier, inc=1, device_id=device, device_id_type=MESH)

    plane = PLANE_FAR
    for n, (dy, dx) in enumerate(plane):
        greet((z, 2 * chip_at(dy, dx) + k))
        if n < len(Z_FAR):
            oz = lax.rem(z + Z_FAR[n], Z)
            greet((oz, c))
            greet((oz, partner))
    greet((z, partner))

    lab_at = (
        pl.ds(pl.multiple_of(k * OUTS + y * 8, 8), 8),
        pl.ds(pl.multiple_of(x * RS_ROWS, RS_ROWS), RS_ROWS),
    )
    loads = [
        pltpu.make_async_copy(feat_hbm, feat, load_sem.at[0]),
        pltpu.make_async_copy(cent_hbm, cent.at[k], load_sem.at[1]),
        pltpu.make_async_copy(coef_hbm, coef, load_sem.at[2]),
        pltpu.make_async_copy(lab_hbm.at[lab_at], lab, load_sem.at[3]),
        pltpu.make_async_copy(prec_hbm, p_raw.at[k], load_sem.at[4]),
    ]
    for copy in loads:
        copy.start()

    def remote(src, dst, send, recv, device):
        return pltpu.make_async_remote_copy(
            src_ref=src, dst_ref=dst, send_sem=send, recv_sem=recv, device_id=device, device_id_type=MESH
        )

    def to_pair(src, dst, n):
        return remote(src, dst, pair_send.at[n], pair_recv.at[n], (z, partner))

    def to_plane(src, dst, ss, rs, dy, dx):
        o = dy * X + dx
        return remote(src, dst, ss.at[o], rs.at[o], (z, 2 * chip_at(dy, dx) + k))

    def to_z(src, dst, ss, rs, oz):
        return remote(src, dst, ss.at[oz], rs.at[oz], (lax.rem(z + oz, Z), c))

    factor = 2.0 * LOG2E / D
    loads[0].wait()
    fx = feat[...]
    hi, mid, lo = split3(fx)
    r1[...] = jnp.concatenate([hi, hi], axis=1)
    r2[...] = jnp.concatenate([mid, mid], axis=1)
    r3[...] = jnp.concatenate([lo, hi], axis=1)
    hi, mid, lo = split3(fx * fx)
    ones = jnp.ones((16, D), bf16)
    row_norm = dot(ones, hi, 1) + dot(ones, mid, 1) + dot(ones, lo, 1)
    norm[...] = row_norm[:8] * factor

    def kernel_half(h):
        cx = cent[h]
        hi, mid, lo = split3(cx)
        l1[...] = jnp.concatenate([hi, mid], axis=1)
        l2[...] = jnp.concatenate([hi, lo], axis=1)
        cn = jnp.sum(cx * cx, axis=1, keepdims=True) * factor

        @pl.loop(0, X)
        def _(i):
            at = pl.ds(pl.multiple_of(i * RS_ROWS, RS_ROWS), RS_ROWS)
            cross = dot(l1[...], r1[at, :], 1) + dot(l1[...], r2[at, :], 1) + dot(l2[...], r3[at, :], 1)
            tile = jnp.exp2(cross * (2.0 * factor) - (cn + norm[:1, at]))
            hi, lo = split(tile)
            k_hi[h, :, at] = hi
            k_lo[h, :, at] = lo
            hi, lo = split(tile.T)
            kt_hi[h, at, :] = hi
            kt_lo[h, at, :] = lo

    def precond_half(h):
        @pl.loop(0, PROWS // 128)
        def _(i):
            at = pl.multiple_of(i * 128, 128)
            tile = p_raw[h, pl.ds(at, 128), :]
            hi, lo = split(tile)
            p_hi[h, pl.ds(at, 128), :] = hi
            p_lo[h, pl.ds(at, 128), :] = lo
            hi, lo = split(tile.T)
            pt_hi[h, :, pl.ds(at, 128)] = hi
            pt_lo[h, :, pl.ds(at, 128)] = lo

    precond_chunks = [
        remote(
            p_raw.at[k, pl.ds(i * 256, 256), :], p_raw.at[k, pl.ds(i * 256, 256), :],
            pch_send.at[i], pch_recv.at[i], (z, partner),
        )
        for i in range(8)
    ]

    loads[1].wait()
    kernel_half(k)
    loads[2].wait()

    def line_of(pieces, rg):
        return jnp.concatenate([pieces[og * X + rg] for og in range(GROUPS)], axis=0)

    def half_of(pieces, h):
        return jnp.concatenate([pieces[h * (Z // 2) + i] for i in range(Z // 2)], axis=1)

    def pair_of(pieces, p):
        return jnp.concatenate([pieces[2 * p], pieces[2 * p + 1]], axis=1)

    def pair_at(p):
        return p // 2, pl.ds(pl.multiple_of((p % 2) * PAIR, PAIR), PAIR)

    def row_block(dx, size):
        rg = lax.rem(x + dx, X)
        return rg, pl.ds(pl.multiple_of(rg * size, size), size)

    def scatter_plane(pieces, landing, ss, rs, dx):
        for dy in FAR_FIRST:
            if (dy, dx) != (0, 0):
                to_plane(pieces.at[chip_at(dy, dx)], landing.at[dy * X + dx], ss, rs, dy, dx).start()

    def plane_sum(pieces, landing, ss, rs):
        total = pieces[j]
        for dy, dx in reversed(plane):
            to_plane(pieces.at[j], landing.at[dy * X + dx], ss, rs, dy, dx).wait_recv()
            total = total + landing[dy * X + dx]
        return total

    def gather_plane(pieces, ss, rs):
        for dy, dx in plane:
            to_plane(pieces.at[j], pieces.at[j], ss, rs, dy, dx).start()

    def arrived_line(pieces, ss, rs, dx):
        for dy in reversed(FAR_FIRST):
            if (dy, dx) != (0, 0):
                to_plane(pieces.at[j], pieces.at[chip_at(Y - dy, X - dx)], ss, rs, dy, dx).wait_recv()

    def sent_plane(pieces, ss, rs):
        for dy, dx in plane:
            to_plane(pieces.at[j], pieces.at[j], ss, rs, dy, dx).wait_send()

    def pair_members(r):
        p = lax.rem(zp + r, PAIRS)
        return p, ([2 * p, 2 * p + 1] if r else [z + 1 - 2 * zlo])

    def scatter_z(pieces, landing, ss, rs, r):
        for other_z in pair_members(r)[1]:
            oz = lax.rem(other_z - z + Z, Z)
            to_z(pieces.at[other_z], landing.at[oz], ss, rs, oz).start()

    def z_sum(pieces, landing, ss, rs):
        total = pieces[z]
        for oz in reversed(Z_FAR):
            to_z(pieces.at[z], landing.at[oz], ss, rs, oz).wait_recv()
            total = total + landing[oz]
        return total

    def gather_z(pieces, ss, rs):
        for oz in Z_FAR:
            to_z(pieces.at[z], pieces.at[z], ss, rs, oz).start()

    def arrived_pair(pieces, ss, rs, r):
        for other_z in pair_members(r)[1]:
            to_z(pieces.at[z], pieces.at[other_z], ss, rs, lax.rem(z - other_z + Z, Z)).wait_recv()

    def sent_z(pieces, ss, rs):
        for oz in Z_FAR:
            to_z(pieces.at[z], pieces.at[z], ss, rs, oz).wait_send()

    def send_logits(dx, part):
        rg = lax.rem(x + dx, X)
        for og in range(GROUPS):
            log_p[og * X + rg] = part[og * 8 : og * 8 + 8]
        scatter_plane(log_p, log_r, log_ss, log_rs, dx)

    lhs = stacked(jnp.concatenate([coef[pl.ds(theirs, OUTS), :], coef[pl.ds(mine, OUTS), :]], axis=0))
    for n, dx in enumerate(FAR_FIRST):
        rg, at = row_block(dx, RS_ROWS)
        part = product(lhs, k_hi[k, :, at], k_lo[k, :, at], 0)
        pair_s[n] = part[:OUTS]
        log_a[n] = part[OUTS:]
    pl.semaphore_wait(barrier, 1 + len(plane) + 2 * (Z - 1))
    pairs = [to_pair(pair_s.at[n], pair_r.at[n], n) for n in range(X)]
    for copy in pairs:
        copy.start()
    cent_pair = to_pair(cent.at[k], cent.at[k], 4)
    cent_pair.start()
    coef_copy = to_pair(coef.at[pl.ds(theirs, OUTS), :], coef_pair, 5)
    coef_copy.start()
    for n, dx in enumerate(FAR_FIRST):
        pairs[n].wait_recv()
        send_logits(dx, log_a[n] + pair_r[n])
    loads[4].wait()
    for copy in precond_chunks[:4]:
        copy.start()
    for copy in pairs:
        copy.wait_send()
    cent_pair.wait()
    kernel_half(other)
    coef_copy.wait()
    for i in range(CENT // PIECE):
        col = slice(i * PIECE, i * PIECE + PIECE)
        a_f[k * (Z // 2) + i] = coef[pl.ds(mine, OUTS), col]
        a_f[other * (Z // 2) + i] = coef_pair[:, col]
    precond_half(k)
    loads[3].wait()

    @pl.loop(0, STEPS)
    def _(step):
        total = plane_sum(log_p, log_r, log_ss, log_rs)
        res_f[j] = (jax.nn.sigmoid(total) - lab[...].astype(f32)) * (1.0 / (ROWS * Z))
        gather_plane(res_f, res_ss, res_rs)

        @pl.when(step == 0)
        def _():
            for copy in precond_chunks[4:]:
                copy.start()

        sent_plane(log_p, log_ss, log_rs)

        for dx in NEAR_FIRST:
            arrived_line(res_f, res_ss, res_rs, dx)
            rg, rows = row_block(X - dx, RS_ROWS)
            lhs = stacked(line_of(res_f, rg))
            for n, r in enumerate(FAR_FIRST):
                p = lax.rem(zp + r, PAIRS)
                h, at = pair_at(p)
                part = product(lhs, kt_hi[h, rows, at], kt_lo[h, rows, at], 0)
                if dx != NEAR_FIRST[0]:
                    part = col_a[n] + part
                if dx != NEAR_FIRST[-1]:
                    col_a[n] = part
                else:
                    gra_p[2 * p] = part[:, :PIECE]
                    gra_p[2 * p + 1] = part[:, PIECE:]
                    scatter_z(gra_p, gra_r, gra_ss, gra_rs, r)
        sent_plane(res_f, res_ss, res_rs)

        @pl.when(step == 0)
        def _():
            for copy in precond_chunks:
                copy.wait()
            precond_half(other)

        gra_f[z] = z_sum(gra_p, gra_r, gra_ss, gra_rs)
        gather_z(gra_f, grf_ss, grf_rs)
        sent_z(gra_p, gra_ss, gra_rs)

        for r in NEAR_FIRST:
            arrived_pair(gra_f, grf_ss, grf_rs, r)
        halves = [stacked(half_of(gra_f, h)) for h in range(2)]
        for dx in FAR_FIRST:
            rg, rows = row_block(dx, RS_PROWS)
            part = sum(product(halves[h], pt_hi[h, :, rows], pt_lo[h, :, rows], 0) for h in range(2))
            for og in range(GROUPS):
                fwd_p[og * X + rg] = part[og * 8 : og * 8 + 8]
            scatter_plane(fwd_p, fwd_r, fwd_ss, fwd_rs, dx)
        sent_z(gra_f, grf_ss, grf_rs)
        fwd_f[j] = plane_sum(fwd_p, fwd_r, fwd_ss, fwd_rs)
        gather_plane(fwd_f, fwf_ss, fwf_rs)
        sent_plane(fwd_p, fwd_ss, fwd_rs)

        def square_to(oz, r):
            n = oz * 2 + r
            return remote(
                sq_s.at[step], sq_r.at[step, n], sq_ss.at[step, n], sq_rs.at[step, n],
                (lax.rem(z + oz, Z), partner if r else c),
            )

        square = jnp.zeros((8, 128), f32)
        for dx in NEAR_FIRST:
            arrived_line(fwd_f, fwf_ss, fwf_rs, dx)
            rg, rows = row_block(X - dx, RS_PROWS)
            line = line_of(fwd_f, rg)
            for og in range(GROUPS):
                for t in range(RS_PROWS // 128):
                    tile = line[og * 8 : og * 8 + 8, t * 128 : t * 128 + 128]
                    square = square + tile * tile
            if dx == NEAR_FIRST[-1]:
                square = jnp.sum(square, axis=0, keepdims=True)
                sq_s[step] = square
                for oz, r in RING:
                    square_to(oz, r).start()
            lhs = stacked(line)
            for n, r in enumerate(FAR_FIRST):
                p = lax.rem(zp + r, PAIRS)
                h, at = pair_at(p)
                part = product(lhs, p_hi[h, rows, at], p_lo[h, rows, at], 0)
                if dx != NEAR_FIRST[0]:
                    part = col_a[n] + part
                if dx != NEAR_FIRST[-1]:
                    col_a[n] = part
                else:
                    bak_p[2 * p] = part[:, :PIECE]
                    bak_p[2 * p + 1] = part[:, PIECE:]
                    scatter_z(bak_p, bak_r, bak_ss, bak_rs, r)
        sent_plane(fwd_f, fwf_ss, fwf_rs)
        for oz, r in reversed(RING):
            square_to(oz, r).wait_recv()
            square = square + sq_r[step, oz * 2 + r]
        square = jnp.sum(square, axis=1, keepdims=True)
        scale = step_size / jnp.sqrt(square / (CENT * 2 * CHIPS * OUT) + epsilon)
        a_f[z] = a_f[z] - scale * z_sum(bak_p, bak_r, bak_ss, bak_rs)

        @pl.when(step < STEPS - 1)
        def _():
            gather_z(a_f, af_ss, af_rs)

        sent_z(bak_p, bak_ss, bak_rs)
        for oz, r in RING:
            square_to(oz, r).wait_send()

        @pl.when(step < STEPS - 1)
        def _():
            for r in NEAR_FIRST:
                arrived_pair(a_f, af_ss, af_rs, r)
            halves = [stacked(half_of(a_f, h)) for h in range(2)]
            for dx in FAR_FIRST:
                rg, rows = row_block(dx, RS_ROWS)
                send_logits(dx, sum(product(halves[h], k_hi[h, :, rows], k_lo[h, :, rows], 0) for h in range(2)))
            sent_z(a_f, af_ss, af_rs)

    holder = z // (Z // 2)
    rel = lax.rem(k + holder, 2)

    def to_holder(oz, r):
        return remote(
            a_f.at[z], fin.at[k * (Z // 2) + lax.rem(z, Z // 2)], fin_ss.at[oz], fin_rs.at[oz * 2 + r],
            (lax.rem(z + oz, Z), 2 * j + holder),
        )

    copies = [to_holder(oz, rel) for oz in Z_FAR]
    for copy in copies:
        copy.start()

    @pl.when(rel == 0)
    def _():
        fin[k * (Z // 2) + lax.rem(z, Z // 2)] = a_f[z]

    @pl.when(rel == 1)
    def _():
        to_holder(0, 1).start()
        to_holder(0, 1).wait_send()

    for i in range(Z // 2):
        source = k * (Z // 2) + i
        oz = lax.rem(z - source + Z, Z)

        def arrived(r):
            owner = k + r * (1 - 2 * k)
            remote(
                a_f.at[z], fin.at[owner * (Z // 2) + i], fin_ss.at[oz], fin_rs.at[oz * 2 + r], (z, partner)
            ).wait_recv()

        pl.when(source != z)(functools.partial(arrived, 0))
        arrived(1)
    for copy in copies:
        copy.wait_send()
    for n in range(2):
        for i in range(Z // 2):
            out_ref[n * OUTS : n * OUTS + OUTS, i * PIECE : i * PIECE + PIECE] = fin[n * (Z // 2) + i]


def body(features, centers, labels, coeffs, precond):
    any_space = pl.BlockSpec(memory_space=pl.ANY)
    V = pltpu.VMEM
    dma = pltpu.SemaphoreType.DMA
    scratch = [
        V((ROWS, D), f32),
        V((2, CENT, D), f32),
        V((8, RS_ROWS), jnp.int32),
        V((OUT, CENT), f32),
        V((OUTS, CENT), f32),
        V((ROWS, 2 * D), bf16),
        V((ROWS, 2 * D), bf16),
        V((ROWS, 2 * D), bf16),
        V((CENT, 2 * D), bf16),
        V((CENT, 2 * D), bf16),
        V((8, ROWS), f32),
        V((2, CENT, ROWS), bf16),
        V((2, CENT, ROWS), bf16),
        V((2, ROWS, CENT), bf16),
        V((2, ROWS, CENT), bf16),
        V((2, PROWS, CENT), f32),
        V((2, PROWS, CENT), bf16),
        V((2, PROWS, CENT), bf16),
        V((2, CENT, PROWS), bf16),
        V((2, CENT, PROWS), bf16),
        V((X, OUTS, RS_ROWS), f32),
        V((X, OUTS, RS_ROWS), f32),
        V((X, OUTS, RS_ROWS), f32),
        V((PAIRS, OUTS, PAIR), f32),
        V((X, OUTS, RS_PROWS), f32),
        V((CHIPS, 8, RS_ROWS), f32),
        V((CHIPS, 8, RS_ROWS), f32),
        V((CHIPS, 8, RS_ROWS), f32),
        V((Z, OUTS, PIECE), f32),
        V((Z, OUTS, PIECE), f32),
        V((Z, OUTS, PIECE), f32),
        V((CHIPS, 8, RS_PROWS), f32),
        V((CHIPS, 8, RS_PROWS), f32),
        V((CHIPS, 8, RS_PROWS), f32),
        V((Z, OUTS, PIECE), f32),
        V((Z, OUTS, PIECE), f32),
        V((Z, OUTS, PIECE), f32),
        V((STEPS, 1, 128), f32),
        V((STEPS, 2 * Z, 1, 128), f32),
        V((Z, OUTS, PIECE), f32),
        dma((5,)),
        dma((9,)),
        dma((9,)),
        dma((8,)),
        dma((8,)),
    ]
    for count in (CHIPS, CHIPS, Z, Z, CHIPS, CHIPS, Z, Z):
        scratch += [dma((count,)), dma((count,))]
    scratch += [dma((STEPS, 2 * Z)), dma((STEPS, 2 * Z)), dma((Z,)), dma((2 * Z,))]
    out = pl.pallas_call(
        kernel,
        out_shape=pltpu.VMEM((OUT, CENT), f32),
        in_specs=[any_space] * 5,
        out_specs=pl.BlockSpec(memory_space=pltpu.VMEM),
        scratch_shapes=scratch,
        compiler_params=pltpu.CompilerParams(
            collective_id=0, has_side_effects=True, vmem_limit_bytes=60 * 1024 * 1024
        ),
        name="falkon",
    )(features, centers, labels.T, coeffs.T, precond)
    return out.T


def solution(mesh):
    in_specs = (
        P("rows", None),
        P("centers", None),
        P("rows", None),
        P("centers", None),
        P("rows", "centers"),
    )
    return jax.shard_map(body, mesh=mesh, in_specs=in_specs, out_specs=P("centers", None), check_vma=False)
```
